768 devices in a mesh: gx: 128 (over z_hi, y, x, core), gz: 6 (over z_lo).
Axes of the slice: x: 4, y: 8, z: 12 (z_hi: 2, z_lo: 6; z = z_hi * 6 + z_lo), core: 2. Of those that a mesh axis runs over, the one named last changes fastest.
Arguments:
- state: float32 [5, 1024, 16, 768], P(None, 'gx', None, 'gz'), may hold values from -1 to 8.5, as said below
- register: float32 [5, 1024, 16, 768], P(None, 'gx', None, 'gz'), may hold values from -2.4 to 2.4
- top_ghost: float32 [5, 1024, 3, 768], P(None, 'gx', None, 'gz'), may hold values from -1 to 8.5, as said below
- flags: int32 [1024, 16, 6], P('gx', None, 'gz'), may hold values 0 or 1
Outputs:
- new_state: float32 [5, 1024, 16, 768], P(None, 'gx', None, 'gz')
- new_register: float32 [5, 1024, 16, 768], P(None, 'gx', None, 'gz')
The draws below stay inside these ranges and needn't reach their ends.
Inputs may be any that keep to these rules, and one draw needn't show every extreme that they name: `state`: conserved variables of an ideal gas with ratio of heats 1.4, density 0.5 to 2 and pressure 0.3 to 1.5 in every cell. `top_ghost`: conserved variables of an ideal gas with ratio of heats 1.4, density 0.5 to 2 and pressure 0.3 to 1.5 in every cell.
All inputs are finite; a program needn't handle non-finite values. No bound on the sum of `flags` on one device may be relied on, other than what follows from the above.
Results may differ from the reference program's by a relative error of at most 0.0003.
Values sent between devices are 32-bit elements; how exact they have to be, the bound alone decides.
No kernel may reach another device: no remote copies, remote signals or barrier semaphores. Data moves between devices by JAX's collectives and lax.ppermute only.
A program may use at most 32 MiB of HBM per device.

```python
import math
import jax
import jax.numpy as jnp
from jax import lax

CX = 8
NY = 16
CZ = 128
ZBLOCK = 128
NX = 1024
NZ = 768
N_GX = 128


def speed_levels(key):
    keys = jax.random.split(jax.random.fold_in(key, 31), 2)
    stream_count = NX // CX
    span_count = NZ // CZ
    base = jax.random.uniform(keys[0], (stream_count,), jnp.float32, 0.0, 1.0)
    stream_level = 0.6 + 0.4 * base * base * base * base
    span_level = jax.random.uniform(keys[1], (span_count,), jnp.float32, 0.6, 1.0)
    stream_cells = jnp.repeat(stream_level, CX, total_repeat_length=NX)
    span_cells = jnp.repeat(span_level, CZ, total_repeat_length=NZ)
    return stream_cells[:, None, None] * span_cells[None, None, :]


def gas_state(key, shape, level):
    keys = jax.random.split(key, 5)
    density = jnp.exp(jax.random.uniform(keys[0], shape, jnp.float32, math.log(0.5), math.log(2.0)))
    vel_x = jax.random.uniform(keys[1], shape, jnp.float32, 0.4, 2.0)
    vel_y = jax.random.uniform(keys[2], shape, jnp.float32, -0.5, 0.5)
    vel_z = jax.random.uniform(keys[3], shape, jnp.float32, -0.5, 0.5)
    pressure = jnp.exp(jax.random.uniform(keys[4], shape, jnp.float32, math.log(0.3), math.log(1.5)))
    vel_x = vel_x * level
    vel_y = vel_y * level
    vel_z = vel_z * level
    energy = pressure / 0.4 + 0.5 * density * (vel_x * vel_x + vel_y * vel_y + vel_z * vel_z)
    return jnp.stack([density, density * vel_x, density * vel_y, density * vel_z, energy])


def draw_state(key, part):
    return gas_state(jax.random.fold_in(key, 11), (NX, NY, NZ), speed_levels(key))


def draw_top_ghost(key, part):
    return gas_state(jax.random.fold_in(key, 23), (NX, 3, NZ), speed_levels(key))


def set_ends(result, key, low, largest):
    shape = result.shape
    spot = [jax.random.randint(jax.random.fold_in(key, axis), (), 0, shape[axis]) for axis in range(len(shape))]
    result = result.at[tuple(spot)].set(low)
    longest = shape.index(max(shape))
    spot[longest] = (spot[longest] + 1) % shape[longest]
    return result.at[tuple(spot)].set(largest)


def level_of(stream_key, dims, cuts, smallest, top_value):
    loudness, own = 1.0, jax.random.fold_in(stream_key, 6)
    for dim, blocks in cuts:
        heights = jnp.exp(jax.random.uniform(jax.random.fold_in(own, dim), (blocks,), jnp.float32, smallest / len(cuts), top_value / len(cuts)))
        loudness = loudness * jnp.repeat(heights, dims[dim] // blocks).reshape([-1 if axis == dim else 1 for axis in range(len(dims))])
    return loudness


def normal_values(key, extent, spread, reach, cuts=(), kind=jnp.bfloat16):
    factor_of = level_of(key, extent, cuts, -0.22, 0.18) if cuts else 1.0
    result = jax.random.normal(key, extent, jnp.float32) * spread * factor_of
    return jnp.minimum(jnp.maximum(result, -reach), reach).astype(kind)


def setup_inputs(seed: int = 0) -> dict:
    streams_of = jax.random.split(jax.random.key(seed), 5)
    return {
        "state": draw_state(jax.random.fold_in(streams_of[4], 71), 0),
        "register": normal_values(streams_of[1], (5, NX, NY, NZ), 0.4, 2.4, ((1, 128), (3, 6)), jnp.float32),
        "top_ghost": draw_top_ghost(jax.random.fold_in(streams_of[4], 71), 0),
        "flags": set_ends((jax.random.randint(streams_of[3], (NX, NY, NZ // ZBLOCK), 0, 2) < 1).astype(jnp.int32), jax.random.fold_in(streams_of[3], 1), 0, 1),
    }


GAMMA = 1.4
EPS_WENO = 1e-06
LAMBDA_X = 0.1
LAMBDA_Y = 0.15
LAMBDA_Z = 0.1
REGISTER_DECAY = -5.0 / 9.0
UPDATE_WEIGHT = 15.0 / 16.0

def primitives(cons):
    density = cons[0]
    inverse = 1.0 / density
    vel_x = cons[1] * inverse
    vel_y = cons[2] * inverse
    vel_z = cons[3] * inverse
    pressure = (GAMMA - 1.0) * (cons[4] - 0.5 * (cons[1] * vel_x + cons[2] * vel_y + cons[3] * vel_z))
    return (density, vel_x, vel_y, vel_z, pressure)

def local_speeds(prims):
    density, vel_x, vel_y, vel_z, pressure = prims
    sound = jnp.sqrt(GAMMA * pressure / density)
    return jnp.stack([jnp.max(jnp.abs(vel_x) + sound), jnp.max(jnp.abs(vel_y) + sound), jnp.max(jnp.abs(vel_z) + sound)])

def physical_flux(cons, prims, var):
    pressure = prims[4]
    velocity = prims[var]
    rows = [cons[0] * velocity, cons[1] * velocity, cons[2] * velocity, cons[3] * velocity, (cons[4] + pressure) * velocity]
    rows[var] = rows[var] + pressure
    return jnp.stack(rows)

def weno_face(vals):
    first, second, third, fourth, fifth = vals
    cand_a = (2.0 * first - 7.0 * second + 11.0 * third) / 6.0
    cand_b = (-second + 5.0 * third + 2.0 * fourth) / 6.0
    cand_c = (2.0 * third + 5.0 * fourth - fifth) / 6.0
    smooth_a = 13.0 / 12.0 * (first - 2.0 * second + third) ** 2 + 0.25 * (first - 4.0 * second + 3.0 * third) ** 2
    smooth_b = 13.0 / 12.0 * (second - 2.0 * third + fourth) ** 2 + 0.25 * (second - fourth) ** 2
    smooth_c = 13.0 / 12.0 * (third - 2.0 * fourth + fifth) ** 2 + 0.25 * (3.0 * third - 4.0 * fourth + fifth) ** 2
    weight_a = 0.1 / (EPS_WENO + smooth_a) ** 2
    weight_b = 0.6 / (EPS_WENO + smooth_b) ** 2
    weight_c = 0.3 / (EPS_WENO + smooth_c) ** 2
    return (weight_a * cand_a + weight_b * cand_b + weight_c * cand_c) / (weight_a + weight_b + weight_c)

def divergence(padded, prims, alpha, var, axis_pos, count, cell_flag):
    flux = physical_flux(padded, prims, var)
    plus = 0.5 * (flux + alpha * padded)
    minus = 0.5 * (flux - alpha * padded)

    def window(arr, offset):
        return lax.slice_in_dim(arr, offset, offset + count + 1, axis=axis_pos)
    central = (37.0 * (window(flux, 2) + window(flux, 3)) - 8.0 * (window(flux, 1) + window(flux, 4)) + (window(flux, 0) + window(flux, 5))) / 60.0
    upwind = weno_face([window(plus, 0), window(plus, 1), window(plus, 2), window(plus, 3), window(plus, 4)])
    upwind = upwind + weno_face([window(minus, 5), window(minus, 4), window(minus, 3), window(minus, 2), window(minus, 1)])

    def jump(face):
        return lax.slice_in_dim(face, 1, count + 1, axis=axis_pos) - lax.slice_in_dim(face, 0, count, axis=axis_pos)
    return jnp.where(cell_flag[None], jump(upwind), jump(central))

def wall_pad(inner, top_ghost):
    mirror = jnp.array([1.0, 1.0, -1.0, 1.0, 1.0], dtype=jnp.float32).reshape(5, 1, 1, 1)
    lower = jnp.flip(inner[:, :, :3], axis=2) * mirror
    return jnp.concatenate([lower, inner, top_ghost], axis=2)

def expand_flags(flags):
    shape = flags.shape
    wide = jnp.broadcast_to(flags[:, :, :, None], (shape[0], shape[1], shape[2], ZBLOCK))
    return wide.reshape(shape[0], shape[1], shape[2] * ZBLOCK) > 0

def advance(inner, x_pad, z_pad, y_pad, register, cell_flag, alpha, x_prims):
    div_x = divergence(x_pad, x_prims, alpha[0], 1, 1, inner.shape[1], cell_flag)
    div_y = divergence(y_pad, primitives(y_pad), alpha[1], 2, 2, inner.shape[2], cell_flag)
    div_z = divergence(z_pad, primitives(z_pad), alpha[2], 3, 3, inner.shape[3], cell_flag)
    change = -(LAMBDA_X * div_x + LAMBDA_Y * div_y + LAMBDA_Z * div_z)
    new_register = REGISTER_DECAY * register + change
    new_state = inner + UPDATE_WEIGHT * new_register
    return (new_state, new_register)

def reference(state, register, top_ghost, flags):
    blocks = jnp.arange(N_GX, dtype=jnp.int32)

    def block_speeds(index):
        inner = lax.dynamic_slice_in_dim(state, index * CX, CX, 1)
        return local_speeds(primitives(inner))
    alpha = lax.optimization_barrier(jnp.max(lax.map(block_speeds, blocks), axis=0))

    def block_update(index):
        start = index * CX
        rows = (start - 3 + jnp.arange(CX + 6, dtype=jnp.int32)) % NX
        x_pad = jnp.take(state, rows.astype(jnp.int32), axis=1)
        inner = lax.dynamic_slice_in_dim(state, start, CX, 1)
        reg_block = lax.dynamic_slice_in_dim(register, start, CX, 1)
        top_block = lax.dynamic_slice_in_dim(top_ghost, start, CX, 1)
        flag_block = lax.dynamic_slice_in_dim(flags, start, CX, 0)
        z_pad = jnp.concatenate([inner[:, :, :, NZ - 3:], inner, inner[:, :, :, :3]], axis=3)
        y_pad = wall_pad(inner, top_block)
        return advance(inner, x_pad, z_pad, y_pad, reg_block, expand_flags(flag_block), alpha, primitives(x_pad))
    states, registers = lax.map(block_update, blocks)
    new_state = jnp.moveaxis(states, 0, 1).reshape(5, NX, NY, NZ)
    new_register = jnp.moveaxis(registers, 0, 1).reshape(5, NX, NY, NZ)
    return (new_state, new_register)
```

```python
import functools

import jax
import jax.numpy as jnp
from jax import lax
from jax.sharding import Mesh
from jax.sharding import PartitionSpec as P

ZBLOCK = 128
GX_GZ = ("gx_0", "gx_1", "gx_2", "gx_3", "gz")
GX = ("gx_0", "gx_1", "gx_2", "gx_3")


GAMMA = 1.4
EPS_WENO = 1e-06
LAMBDA_X = 0.1
LAMBDA_Y = 0.15
LAMBDA_Z = 0.1
REGISTER_DECAY = -5.0 / 9.0
UPDATE_WEIGHT = 15.0 / 16.0


def max_over(value, axes):
    size = functools.reduce(lambda a, b: a * b, [lax.axis_size(a) for a in axes])
    sent = jnp.broadcast_to(value[None], (size, value.shape[0]))
    return jnp.max(lax.all_to_all(sent, axes, 0, 0, tiled=True), axis=0)


def by_axis(value, axes):
    return max_over(max_over(value, ("gx_1", "gx_2", "gx_3")), ("gx_0", "gz"))


def with_halo(value, sides, width):
    edges = {}
    for axis, dim in sides:
        size, length = (lax.axis_size(axis), value.shape[dim])
        up = [(i, (i + 1) % size) for i in range(size)]
        last = lax.slice_in_dim(value, length - width, length, axis=dim)
        first = lax.slice_in_dim(value, 0, width, axis=dim)
        edges[dim] = (
            lax.ppermute(last, axis, up),
            lax.ppermute(first, axis, [(b, a) for a, b in up]),
        )
    done = []
    for _, dim in sides:
        low, high = edges[dim]
        around = [(width, width) if d in done else (0, 0) for d in range(value.ndim)]
        value = jnp.concatenate([jnp.pad(low, around), value, jnp.pad(high, around)], axis=dim)
        done.append(dim)
    return value


def primitives(cons):
    density = cons[0]
    inverse = 1.0 / density
    vel_x = cons[1] * inverse
    vel_y = cons[2] * inverse
    vel_z = cons[3] * inverse
    pressure = (GAMMA - 1.0) * (
        cons[4] - 0.5 * (cons[1] * vel_x + cons[2] * vel_y + cons[3] * vel_z)
    )
    return (density, vel_x, vel_y, vel_z, pressure)


def global_speeds(prims):
    density, vel_x, vel_y, vel_z, pressure = prims
    sound = jnp.sqrt(GAMMA * pressure / density)
    local = jnp.stack(
        [
            jnp.max(jnp.abs(vel_x) + sound),
            jnp.max(jnp.abs(vel_y) + sound),
            jnp.max(jnp.abs(vel_z) + sound),
        ]
    )
    return by_axis(local, GX_GZ)


def physical_flux(cons, prims, var):
    pressure = prims[4]
    velocity = prims[var]
    rows = [
        cons[0] * velocity,
        cons[1] * velocity,
        cons[2] * velocity,
        cons[3] * velocity,
        (cons[4] + pressure) * velocity,
    ]
    rows[var] = rows[var] + pressure
    return jnp.stack(rows)


def weno_face(vals):
    first, second, third, fourth, fifth = vals
    cand_a = (2.0 * first - 7.0 * second + 11.0 * third) / 6.0
    cand_b = (-second + 5.0 * third + 2.0 * fourth) / 6.0
    cand_c = (2.0 * third + 5.0 * fourth - fifth) / 6.0
    smooth_a = (
        13.0 / 12.0 * (first - 2.0 * second + third) ** 2
        + 0.25 * (first - 4.0 * second + 3.0 * third) ** 2
    )
    smooth_b = 13.0 / 12.0 * (second - 2.0 * third + fourth) ** 2 + 0.25 * (second - fourth) ** 2
    smooth_c = (
        13.0 / 12.0 * (third - 2.0 * fourth + fifth) ** 2
        + 0.25 * (3.0 * third - 4.0 * fourth + fifth) ** 2
    )
    weight_a = 0.1 / (EPS_WENO + smooth_a) ** 2
    weight_b = 0.6 / (EPS_WENO + smooth_b) ** 2
    weight_c = 0.3 / (EPS_WENO + smooth_c) ** 2
    return (weight_a * cand_a + weight_b * cand_b + weight_c * cand_c) / (
        weight_a + weight_b + weight_c
    )


def divergence(padded, prims, alpha, var, axis_pos, count, cell_flag):
    flux = physical_flux(padded, prims, var)
    plus = 0.5 * (flux + alpha * padded)
    minus = 0.5 * (flux - alpha * padded)

    def window(arr, offset):
        return lax.slice_in_dim(arr, offset, offset + count + 1, axis=axis_pos)

    central = (
        37.0 * (window(flux, 2) + window(flux, 3))
        - 8.0 * (window(flux, 1) + window(flux, 4))
        + (window(flux, 0) + window(flux, 5))
    ) / 60.0
    upwind = weno_face(
        [window(plus, 0), window(plus, 1), window(plus, 2), window(plus, 3), window(plus, 4)]
    )
    upwind = upwind + weno_face(
        [window(minus, 5), window(minus, 4), window(minus, 3), window(minus, 2), window(minus, 1)]
    )

    def jump(face):
        return lax.slice_in_dim(face, 1, count + 1, axis=axis_pos) - lax.slice_in_dim(
            face, 0, count, axis=axis_pos
        )

    return jnp.where(cell_flag[None], jump(upwind), jump(central))


def wall_pad(inner, top_ghost):
    mirror = jnp.array([1.0, 1.0, -1.0, 1.0, 1.0], dtype=jnp.float32).reshape(5, 1, 1, 1)
    lower = jnp.flip(inner[:, :, :3], axis=2) * mirror
    return jnp.concatenate([lower, inner, top_ghost], axis=2)


def expand_flags(flags):
    shape = flags.shape
    wide = jnp.broadcast_to(flags[:, :, :, None], (shape[0], shape[1], shape[2], ZBLOCK))
    return wide.reshape(shape[0], shape[1], shape[2] * ZBLOCK) > 0


def shards(state, register, top_ghost, flags):
    cell_flag = expand_flags(flags)
    both_pad = with_halo(state, ((GX, 1), ("gz", 3)), 3)
    x_pad = both_pad[:, :, :, 3:-3]
    z_pad = both_pad[:, 3:-3]
    y_pad = wall_pad(state, top_ghost)
    x_prims = primitives(x_pad)
    alpha = global_speeds(primitives(state))
    div_x = divergence(x_pad, x_prims, alpha[0], 1, 1, state.shape[1], cell_flag)
    div_y = divergence(y_pad, primitives(y_pad), alpha[1], 2, 2, state.shape[2], cell_flag)
    div_z = divergence(z_pad, primitives(z_pad), alpha[2], 3, 3, state.shape[3], cell_flag)
    change = -(LAMBDA_X * div_x + LAMBDA_Y * div_y + LAMBDA_Z * div_z)
    new_register = REGISTER_DECAY * register + change
    new_state = state + UPDATE_WEIGHT * new_register
    return (new_state, new_register)


def solution(mesh):
    finer = Mesh(
        mesh.devices.reshape(2, 8, 4, 2, mesh.shape["gz"]), ("gx_0", "gx_1", "gx_2", "gx_3", "gz")
    )
    placed = (
        P(None, GX, None, "gz"),
        P(None, GX, None, "gz"),
        P(None, GX, None, "gz"),
        P(GX, None, "gz"),
    )
    return jax.shard_map(
        shards,
        mesh=finer,
        in_specs=placed,
        out_specs=(P(None, GX, None, "gz"), P(None, GX, None, "gz")),
        check_vma=False,
    )
```

```python
import jax
import jax.numpy as jnp
from jax import lax
from jax.experimental import pallas as pl
from jax.experimental.pallas import tpu as pltpu
from jax.sharding import Mesh
from jax.sharding import PartitionSpec as P

GX = ("gx_0", "gx_1", "gx_2", "gx_3")
PLANE = ("gx_1", "gx_2", "gx_3")
ZLINE = ("gx_0", "gz")

GAMMA = 1.4
EPS_WENO = 1e-06
LAMBDA = (0.1, 0.15, 0.1)
REGISTER_DECAY = -5.0 / 9.0
UPDATE_WEIGHT = 15.0 / 16.0

NV = 5
CX = 8
CY = 16
CZ = 128
ROWS = CX * CY
HALO = 3
SUB = 8
LONG = 16 + 2 * HALO
WIDE = CX + 2 * HALO


def primitives(cons):
    inverse = 1.0 / cons[0]
    vels = [cons[k] * inverse for k in (1, 2, 3)]
    kinetic = cons[1] * vels[0] + cons[2] * vels[1] + cons[3] * vels[2]
    pressure = (GAMMA - 1.0) * (cons[4] - 0.5 * kinetic)
    return inverse, vels, pressure


def speed_kernel(state_ref, out_ref):
    best = [None] * 3
    for block in range(ROWS // SUB):
        rows = slice(block * SUB, block * SUB + SUB)
        inverse, vels, pressure = primitives([state_ref[v, rows, :] for v in range(NV)])
        sound = jnp.sqrt(GAMMA * pressure * inverse)
        for k in range(3):
            speed = jnp.abs(vels[k]) + sound
            best[k] = speed if block == 0 else jnp.maximum(best[k], speed)
    lane = lax.broadcasted_iota(jnp.int32, (1, CZ), 1)
    packed = jnp.zeros((1, CZ), jnp.float32)
    for k in range(3):
        top = jnp.max(jnp.max(best[k], axis=0, keepdims=True), axis=1, keepdims=True)
        packed = jnp.where(lane == k, top, packed)
    for to in range(out_ref.shape[0]):
        out_ref[to] = packed


def relay_kernel(got_ref, out_ref):
    best = got_ref[0]
    for i in range(1, got_ref.shape[0]):
        best = jnp.maximum(best, got_ref[i])
    for to in range(out_ref.shape[0]):
        out_ref[to] = best


def edges_kernel(state_ref, turned_ref, first_ref, last_ref):
    for v in range(NV):
        turned = state_ref[v].T
        turned_ref[v] = turned
        first_ref[v] = turned[:HALO]
        last_ref[v] = turned[CZ - HALO :]


def split_flux(cons, var, alpha):
    _, vels, pressure = primitives(cons)
    velocity = vels[var - 1]
    plus, minus = [], []
    for v in range(NV):
        carried = cons[v] + pressure if v == 4 else cons[v]
        flux = carried * velocity
        if v == var:
            flux = flux + pressure
        moved = alpha * cons[v]
        plus.append(flux + moved)
        minus.append(flux - moved)
    return plus, minus


EPS_SCALED = 16.0 * EPS_WENO
CURVE = 13.0 / 3.0


def faces(plus, minus, count):
    total = [p + m for p, m in zip(plus, minus)]

    def slopes(vals):
        step = [b - a for a, b in zip(vals, vals[1:])]
        bend = [None] + [b - a for a, b in zip(step, step[1:])]
        base = [None] + [CURVE * (d * d) + EPS_SCALED for d in bend[1:]]
        return step, bend, base

    pe, pd, pk = slopes(plus)
    me, md, mk = slopes(minus)

    def blend(ta, ka, tb, kb, tc, kc, va, vb, vc):
        ba, bb, bc_ = ka + ta * ta, kb + tb * tb, kc + tc * tc
        x, y, z = bb * bc_, ba * bc_, ba * bb
        wa, wb, wc = x * x, 6.0 * (y * y), 3.0 * (z * z)
        return (wa * va + wb * vb + wc * vc) / (wa + wb + wc)

    ups, cens = [], []
    for j in range(count):
        bc, cd = pe[j + 1], pe[j + 2]
        ta = pd[j + 1] + (bc + bc)
        tb = bc + cd
        tc = pd[j + 3] - (cd + cd)
        up = blend(ta, pk[j + 1], tb, pk[j + 2], tc, pk[j + 3], (ta + ta) - bc, tb + cd, cd - tc)
        bc, cd = me[j + 3], me[j + 2]
        ta = md[j + 4] - (bc + bc)
        tb = bc + cd
        tc = md[j + 2] + (cd + cd)
        down = blend(ta, mk[j + 4], tb, mk[j + 3], tc, mk[j + 2], (ta + ta) + bc, -(tb + cd), -(cd + tc))
        ups.append(6.0 * (plus[j + 2] + minus[j + 3]) + (up + down))
        cens.append(
            37.0 * (total[j + 2] + total[j + 3])
            - 8.0 * (total[j + 1] + total[j + 4])
            + (total[j] + total[j + 5])
        )
    return ups, cens


def jumps(plus, minus, count, masks, scale):
    ups, cens = faces(plus, minus, count + 1)
    return [
        jnp.where(masks[i], (scale / 12.0) * (ups[i + 1] - ups[i]), (scale / 120.0) * (cens[i + 1] - cens[i]))
        for i in range(count)
    ]


def step_kernel(
    speed_ref, state_ref, turned_ref, xlo_ref, xhi_ref, xlo_seam_ref, xhi_seam_ref, zlo_ref, zhi_ref,
    top_ref, flag_ref, reg_ref,
    new_state_ref, new_reg_ref,
    xp, xm, yp, ym, zp, zm, line, mask, acc_y, acc_z,
):
    best = speed_ref[0]
    for i in range(1, speed_ref.shape[0]):
        best = jnp.maximum(best, speed_ref[i])
    lane = lax.broadcasted_iota(jnp.int32, (1, CZ), 1)
    alphas = [jnp.max(jnp.where(lane == k, best, 0.0), axis=1, keepdims=True) for k in range(3)]

    for block in range(ROWS // SUB):
        rows = slice(block * SUB, block * SUB + SUB)
        mask[rows, :] = jnp.broadcast_to(flag_ref[rows, :].astype(jnp.float32), (SUB, CZ))
    turned_mask = mask[...].T[:SUB]

    def x_plane(i, rest_ref, seam_ref, shift):
        for h in range(CY // SUB):
            rows = pl.ds(h * SUB, SUB)
            cons = [rest_ref[v, i, rows, :] + seam_ref[v, i, rows, :] for v in range(NV)]
            plus, minus = split_flux(cons, 1, alphas[0])
            for v in range(NV):
                xp[v, i + shift, rows, :] = plus[v]
                xm[v, i + shift, rows, :] = minus[v]

    for i in range(HALO):
        x_plane(i, xlo_ref, xlo_seam_ref, 0)
        x_plane(i, xhi_ref, xhi_seam_ref, HALO + CX)

    def x_body(i, carry):
        for h in range(CY // SUB):
            rows = pl.ds(pl.multiple_of(i * CY + h * SUB, SUB), SUB)
            plus, minus = split_flux([state_ref[v, rows, :] for v in range(NV)], 1, alphas[0])
            for v in range(NV):
                xp[v, i + HALO, pl.ds(h * SUB, SUB), :] = plus[v]
                xm[v, i + HALO, pl.ds(h * SUB, SUB), :] = minus[v]
        return carry

    lax.fori_loop(0, CX, x_body, 0)

    def y_store(to, cons):
        plus, minus = split_flux(cons, 2, alphas[1])
        for v in range(NV):
            yp[v, to] = plus[v]
            ym[v, to] = minus[v]

    def y_body(i, carry):
        y_store(i + HALO, [state_ref[v, pl.ds(i, CX, stride=CY), :] for v in range(NV)])
        return carry

    lax.fori_loop(0, CY, y_body, 0)
    for i in range(HALO):
        wall = [state_ref[v, pl.ds(i, CX, stride=CY), :] for v in range(NV)]
        wall[2] = -wall[2]
        y_store(HALO - 1 - i, wall)
        y_store(HALO + CY + i, [top_ref[v, i] for v in range(NV)])

    for v in range(NV):
        line[v, :HALO, :] = zlo_ref[v]
        line[v, HALO : HALO + CZ, :] = turned_ref[v]
        line[v, HALO + CZ : 2 * HALO + CZ, :] = zhi_ref[v]

    def z_body(i, carry):
        plus, minus = split_flux([line[v, pl.ds(i, SUB, stride=CZ // SUB), :] for v in range(NV)], 3, alphas[2])
        for v in range(NV):
            zp[v, i] = plus[v]
            zm[v, i] = minus[v]
        return carry

    lax.fori_loop(0, LONG, z_body, 0)

    y_masks = [mask[pl.ds(i, CX, stride=CY), :] > 0.0 for i in range(CY)]
    z_mask = turned_mask > 0.0

    def per_var(v, carry):
        parts = jumps([zp[v, i] for i in range(LONG)], [zm[v, i] for i in range(LONG)], CY, [z_mask] * CY, LAMBDA[2])
        for i in range(CY):
            acc_z[pl.ds(i, SUB, stride=CZ // SUB), :] = parts[i]
        parts = jumps([yp[v, i] for i in range(LONG)], [ym[v, i] for i in range(LONG)], CY, y_masks, LAMBDA[1])
        for i in range(CY):
            acc_y[pl.ds(i, CX, stride=CY), :] = parts[i]
        spread = acc_z[...].T
        for h in range(CY // SUB):
            rows = slice(h * SUB, h * SUB + SUB)
            masks = [mask[i * CY + h * SUB : i * CY + h * SUB + SUB, :] > 0.0 for i in range(CX)]
            parts = jumps(
                [xp[v, i, rows, :] for i in range(WIDE)], [xm[v, i, rows, :] for i in range(WIDE)], CX, masks, LAMBDA[0]
            )
            for i in range(CX):
                at = slice(i * CY + h * SUB, i * CY + h * SUB + SUB)
                change = parts[i] + acc_y[at, :] + spread[at]
                register = REGISTER_DECAY * reg_ref[v, at, :] - change
                new_reg_ref[v, at, :] = register
                new_state_ref[v, at, :] = state_ref[v, at, :] + UPDATE_WEIGHT * register
        return carry

    lax.fori_loop(0, NV, per_var, 0)


def f32(*shape):
    return jax.ShapeDtypeStruct(shape, jnp.float32)


def near(*shape):
    return pltpu.VMEM(shape, jnp.float32)


def held(value):
    return pltpu.with_memory_space_constraint(value, pltpu.VMEM)


def advance(state, register, top_ghost, flags):
    flat = state.reshape(NV, ROWS, CZ)
    halves, n_z = lax.axis_size("gx_0"), lax.axis_size("gz")
    n_plane = lax.axis_size("gx_1") * lax.axis_size("gx_2") * lax.axis_size("gx_3")
    n_x = halves * n_plane

    own = pl.pallas_call(speed_kernel, out_shape=near(halves * n_z, 1, CZ), name="speed")(flat)
    by_line = lax.all_to_all(held(own), ZLINE, 0, 0, tiled=True)
    turned, first, last = pl.pallas_call(
        edges_kernel, out_shape=(near(NV, CZ, ROWS), near(NV, HALO, ROWS), near(NV, HALO, ROWS)), name="edges"
    )(flat)
    relayed = pl.pallas_call(relay_kernel, out_shape=near(n_plane, 1, CZ), name="relay")(held(by_line))
    speeds = lax.all_to_all(held(relayed), PLANE, 0, 0, tiled=True)

    ring = [(i, (i + 1) % n_x) for i in range(n_x)]
    seam = [pair for pair in ring if pair[0] % n_plane == n_plane - 1]
    rest = [pair for pair in ring if pair not in seam]

    def back(pairs):
        return [(b, a) for a, b in pairs]

    upper, lower = state[:, CX - HALO :], state[:, :HALO]
    xlo_seam = lax.ppermute(upper, GX, seam)
    xhi_seam = lax.ppermute(lower, GX, back(seam))
    xlo = lax.ppermute(upper, GX, rest)
    xhi = lax.ppermute(lower, GX, back(rest))
    z_ring = [(i, (i + 1) % n_z) for i in range(n_z)]
    zlo = lax.ppermute(last, "gz", z_ring)
    zhi = lax.ppermute(first, "gz", back(z_ring))

    new_state, new_register = pl.pallas_call(
        step_kernel,
        out_shape=(f32(NV, ROWS, CZ), f32(NV, ROWS, CZ)),
        scratch_shapes=[
            pltpu.VMEM((NV, WIDE, CY, CZ), jnp.float32),
            pltpu.VMEM((NV, WIDE, CY, CZ), jnp.float32),
            pltpu.VMEM((NV, LONG, SUB, CZ), jnp.float32),
            pltpu.VMEM((NV, LONG, SUB, CZ), jnp.float32),
            pltpu.VMEM((NV, LONG, SUB, CZ), jnp.float32),
            pltpu.VMEM((NV, LONG, SUB, CZ), jnp.float32),
            pltpu.VMEM((NV, CZ + 8, ROWS), jnp.float32),
            pltpu.VMEM((ROWS, CZ), jnp.float32),
            pltpu.VMEM((ROWS, CZ), jnp.float32),
            pltpu.VMEM((CZ, ROWS), jnp.float32),
        ],
        name="step",
    )(
        held(speeds), flat, held(turned), held(xlo), held(xhi), held(xlo_seam), held(xhi_seam), held(zlo), held(zhi),
        top_ghost.transpose(0, 2, 1, 3), flags.reshape(ROWS, 1), register.reshape(NV, ROWS, CZ),
    )
    return (new_state.reshape(state.shape), new_register.reshape(state.shape))


def solution(mesh):
    finer = Mesh(
        mesh.devices.reshape(2, 8, 4, 2, mesh.shape["gz"]), ("gx_0", "gx_1", "gx_2", "gx_3", "gz")
    )
    placed = P(None, GX, None, "gz")
    return jax.shard_map(
        advance,
        mesh=finer,
        in_specs=(placed, placed, placed, P(GX, None, "gz")),
        out_specs=(placed, placed),
        check_vma=False,
    )
```

```python
import jax
import jax.numpy as jnp
from jax import lax
from jax.experimental import pallas as pl
from jax.experimental.pallas import tpu as pltpu
from jax.sharding import Mesh
from jax.sharding import PartitionSpec as P

GX = ("gx_0", "gx_1", "gx_2", "gx_3")
PLANE = ("gx_1", "gx_2", "gx_3")
ZLINE = ("gx_0", "gz")

GAMMA = 1.4
EPS_WENO = 1e-06
LAMBDA = (0.1, 0.15, 0.1)
REGISTER_DECAY = -5.0 / 9.0
UPDATE_WEIGHT = 15.0 / 16.0

NV = 5
CX = 8
CY = 16
CZ = 128
ROWS = CX * CY
HALO = 3
SUB = 8
LONG = 16 + 2 * HALO


def primitives(cons):
    inverse = 1.0 / cons[0]
    vels = [cons[k] * inverse for k in (1, 2, 3)]
    kinetic = cons[1] * vels[0] + cons[2] * vels[1] + cons[3] * vels[2]
    pressure = (GAMMA - 1.0) * (cons[4] - 0.5 * kinetic)
    return inverse, vels, pressure


def fetch(pairs, sems):
    copies = [pltpu.make_async_copy(src, dst, sems.at[i]) for i, (src, dst) in enumerate(pairs)]
    for copy in copies:
        copy.start()
    for copy in copies:
        copy.wait()


def line_neighbours():
    n_z, here = lax.axis_size("gz"), lax.axis_index("gz")
    first = lax.axis_index("gx_0") * n_z
    return first + lax.rem(here + n_z - 1, n_z), first + lax.rem(here + 1, n_z)


def open_kernel(far_ref, state_ref, out_ref, sems):
    fetch([(far_ref.at[v], state_ref.at[v]) for v in range(NV)], sems)
    best = [None] * 3
    for block in range(ROWS // SUB):
        rows = slice(block * SUB, block * SUB + SUB)
        inverse, vels, pressure = primitives([state_ref[v, rows, :] for v in range(NV)])
        sound = jnp.sqrt(GAMMA * pressure * inverse)
        for k in range(3):
            speed = jnp.abs(vels[k]) + sound
            best[k] = speed if block == 0 else jnp.maximum(best[k], speed)
    lane = lax.broadcasted_iota(jnp.int32, (1, CZ), 1)
    packed = jnp.zeros((1, CZ), jnp.float32)
    for k in range(3):
        top = jnp.max(jnp.max(best[k], axis=0, keepdims=True), axis=1, keepdims=True)
        packed = jnp.where(lane == k, top, packed)
    firsts, lasts = [], []
    for v in range(NV):
        turned = state_ref[v].T
        firsts.append(turned[:HALO])
        lasts.append(turned[CZ - HALO :])
    _, after = line_neighbours()
    for to in range(out_ref.shape[0]):
        forward = after == to
        for v in range(NV):
            out_ref[to, v * HALO : v * HALO + HALO, :] = jnp.where(forward, lasts[v], firsts[v])
        out_ref[to, NV * HALO : NV * HALO + 1, :] = packed


def relay_kernel(got_ref, out_ref):
    row = slice(NV * HALO, NV * HALO + 1)
    best = got_ref[0, row, :]
    for i in range(1, got_ref.shape[0]):
        best = jnp.maximum(best, got_ref[i, row, :])
    for to in range(out_ref.shape[0]):
        out_ref[to] = best


def flux_of(cons, var):
    _, vels, pressure = primitives(cons)
    velocity = vels[var - 1]
    flux = [(cons[v] + pressure if v == 4 else cons[v]) * velocity for v in range(NV)]
    flux[var] = flux[var] + pressure
    return flux


def linear_parts(flux, cons, masks, scale):
    count = len(flux) - 2 * HALO

    def face(j):
        inner, outer = flux[j + 2] + flux[j + 3], flux[j + 1] + flux[j + 4]
        central = 37.0 * inner - 8.0 * outer + (flux[j] + flux[j + 5])
        return central, 7.0 * inner - outer, (cons[j + 4] - cons[j + 1]) - 3.0 * (cons[j + 3] - cons[j + 2])

    faces = [face(j) for j in range(count + 1)]
    base, tilt = [], []
    for low, high, mask in zip(faces, faces[1:], masks):
        base.append(jnp.where(mask, (scale / 12.0) * (high[1] - low[1]), (scale / 60.0) * (high[0] - low[0])))
        tilt.append(jnp.where(mask, (scale / 12.0) * (high[2] - low[2]), 0.0))
    return base, tilt


EPS_SCALED = 16.0 * EPS_WENO
CURVE = 13.0 / 3.0


def bent_faces(flux, cons, alpha):
    count = len(flux) - 2 * HALO + 1
    moved = [alpha * u for u in cons]

    def slopes(vals):
        step = [b - a for a, b in zip(vals, vals[1:])]
        bend = [None] + [b - a for a, b in zip(step, step[1:])]
        turn = [None] + [b - a for a, b in zip(bend[1:], bend[2:])]
        base = [None] + [CURVE * (d * d) + EPS_SCALED for d in bend[1:]]
        return step, bend, turn, base

    def pull(beta_a, beta_b, beta_c, near_turn, far_turn):
        u, w = beta_b / beta_a, beta_b / beta_c
        u, w = u * u, w * w
        w = 3.0 * w
        return ((u + u) * near_turn + w * far_turn) / (6.0 + u + w)

    pe, pd, pt, pk = slopes([f + m for f, m in zip(flux, moved)])
    me, md, mt, mk = slopes([f - m for f, m in zip(flux, moved)])
    out = []
    for j in range(count):
        bc, cd = pe[j + 1], pe[j + 2]
        ta, tb, tc = pd[j + 1] + (bc + bc), bc + cd, pd[j + 3] - (cd + cd)
        plus = pull(pk[j + 1] + ta * ta, pk[j + 2] + tb * tb, pk[j + 3] + tc * tc, pt[j + 1], pt[j + 2])
        bc, cd = me[j + 3], me[j + 2]
        ta, tb, tc = md[j + 4] - (bc + bc), bc + cd, md[j + 2] + (cd + cd)
        minus = pull(mk[j + 4] + ta * ta, mk[j + 3] + tb * tb, mk[j + 2] + tc * tc, mt[j + 3], mt[j + 2])
        out.append(minus - plus)
    return out


def prepare_kernel(
    state_ref, top_ref, flag_ref, yu_ref, ybase_ref, ytilt_ref, xmask_ref, zmask_ref, yf_ref
):
    square = (CY, CY)
    diagonal = lax.broadcasted_iota(jnp.int32, square, 0) == lax.broadcasted_iota(jnp.int32, square, 1)
    for x in range(CX):
        spread = jnp.broadcast_to(flag_ref[x].astype(jnp.float32), square)
        column = jnp.max(jnp.where(diagonal, spread, 0.0), axis=1, keepdims=True)
        xmask_ref[x * CY : x * CY + CY, :] = jnp.broadcast_to(column, (CY, CZ)) * (LAMBDA[0] / 12.0)
    zmask_ref[...] = xmask_ref[...].T[:SUB] * (LAMBDA[2] / LAMBDA[0])

    def y_store(to, cons):
        flux = flux_of(cons, 2)
        for v in range(NV):
            yf_ref[v, to] = flux[v]
            yu_ref[v, to] = cons[v]

    for i in range(CY):
        cons = [state_ref[v, pl.ds(i, CX, stride=CY), :] for v in range(NV)]
        y_store(i + HALO, cons)
        if i < HALO:
            y_store(HALO - 1 - i, [-c if v == 2 else c for v, c in enumerate(cons)])
            y_store(HALO + CY + i, [top_ref[v, i] for v in range(NV)])

    masks = [xmask_ref[pl.ds(i, CX, stride=CY), :] > 0.0 for i in range(CY)]

    def per_var(v, carry):
        planes = range(LONG)
        base, tilt = linear_parts([yf_ref[v, i] for i in planes], [yu_ref[v, i] for i in planes], masks, LAMBDA[1])
        for i in range(CY):
            ybase_ref[v, i] = base[i]
            ytilt_ref[v, i] = tilt[i]
        return carry

    lax.fori_loop(0, NV, per_var, 0)


def z_kernel(got_ref, state_ref, zmask_ref, zu_ref, zbase_ref, ztilt_ref, zf_ref, line):
    before, after = line_neighbours()
    for v in range(NV):
        rows = slice(v * HALO, v * HALO + HALO)
        line[v, :HALO, :] = got_ref[before, rows, :]
        line[v, HALO : HALO + CZ, :] = state_ref[v].T
        line[v, HALO + CZ : 2 * HALO + CZ, :] = got_ref[after, rows, :]
    for i in range(LONG):
        cons = [line[v, pl.ds(i, SUB, stride=CZ // SUB), :] for v in range(NV)]
        flux = flux_of(cons, 3)
        for v in range(NV):
            zf_ref[v, i] = flux[v]
            zu_ref[v, i] = cons[v]
    mask = zmask_ref[...] > 0.0

    def per_var(v, carry):
        planes = range(LONG)
        base, tilt = linear_parts(
            [zf_ref[v, i] for i in planes], [zu_ref[v, i] for i in planes], [mask] * CY, LAMBDA[2]
        )
        for i in range(CY):
            zbase_ref[v, i] = base[i]
            ztilt_ref[v, i] = tilt[i]
        return carry

    lax.fori_loop(0, NV, per_var, 0)


def step_kernel(
    speed_ref, state_ref, xlo_ref, xhi_ref, xlo_seam_ref, xhi_seam_ref,
    yu_ref, ybase_ref, ytilt_ref, zu_ref, zbase_ref, ztilt_ref, xmask_ref, zmask_ref, old_reg_ref,
    far_state_ref, far_reg_ref,
    ymask_ref, xf_ref, yf_ref, zf_ref, side_f, side_u, acc_y, acc_z, reg_ref, state_out, reg_out, sems,
):
    loads = [pltpu.make_async_copy(old_reg_ref.at[v], reg_ref.at[v], sems.at[2, v]) for v in range(NV)]
    for load in loads:
        load.start()

    best = speed_ref[0]
    for i in range(1, speed_ref.shape[0]):
        best = jnp.maximum(best, speed_ref[i])
    lane = lax.broadcasted_iota(jnp.int32, (1, CZ), 1)
    alphas = [jnp.max(jnp.where(lane == k, best, 0.0), axis=1, keepdims=True) for k in range(3)]
    halves = [slice(h * SUB, h * SUB + SUB) for h in range(CY // SUB)]

    for i in range(HALO):
        for rows in halves:
            for at, rest, seam in ((i, xlo_ref, xlo_seam_ref), (HALO + i, xhi_ref, xhi_seam_ref)):
                cons = [rest[v, i, rows, :] + seam[v, i, rows, :] for v in range(NV)]
                flux = flux_of(cons, 1)
                for v in range(NV):
                    side_f[v, at, rows, :] = flux[v]
                    side_u[v, at, rows, :] = cons[v]

    for i in range(LONG):
        for cons_ref, flux_ref, var in ((yu_ref, yf_ref, 2), (zu_ref, zf_ref, 3)):
            flux = flux_of([cons_ref[v, i] for v in range(NV)], var)
            for v in range(NV):
                flux_ref[v, i] = flux[v]
    for block in range(ROWS // SUB):
        rows = slice(block * SUB, block * SUB + SUB)
        flux = flux_of([state_ref[v, rows, :] for v in range(NV)], 1)
        for v in range(NV):
            xf_ref[v, rows, :] = flux[v]
    for y in range(CY):
        ymask_ref[y] = xmask_ref[pl.ds(y, CX, stride=CY), :] * (LAMBDA[1] / LAMBDA[0])
    for load in loads:
        load.wait()

    def copies(v):
        return [
            pltpu.make_async_copy(state_out.at[v], far_state_ref.at[v], sems.at[0, v]),
            pltpu.make_async_copy(reg_out.at[v], far_reg_ref.at[v], sems.at[1, v]),
        ]

    def per_var(v, carry):
        bent = bent_faces([zf_ref[v, i] for i in range(LONG)], [zu_ref[v, i] for i in range(LONG)], alphas[2])
        for i in range(CY):
            acc_z[pl.ds(i, SUB, stride=CZ // SUB), :] = (
                zbase_ref[v, i] + alphas[2] * ztilt_ref[v, i] + zmask_ref[...] * (bent[i + 1] - bent[i])
            )
        bent = bent_faces([yf_ref[v, i] for i in range(LONG)], [yu_ref[v, i] for i in range(LONG)], alphas[1])
        for i in range(CY):
            acc_y[pl.ds(i, CX, stride=CY), :] = (
                ybase_ref[v, i] + alphas[1] * ytilt_ref[v, i] + ymask_ref[i] * (bent[i + 1] - bent[i])
            )
        spread = acc_z[...].T
        for rows in halves:
            at = [slice(i * CY + rows.start, i * CY + rows.stop) for i in range(CX)]
            flux = (
                [side_f[v, i, rows, :] for i in range(HALO)]
                + [xf_ref[v, here, :] for here in at]
                + [side_f[v, HALO + i, rows, :] for i in range(HALO)]
            )
            cons = (
                [side_u[v, i, rows, :] for i in range(HALO)]
                + [state_ref[v, here, :] for here in at]
                + [side_u[v, HALO + i, rows, :] for i in range(HALO)]
            )
            bent = bent_faces(flux, cons, alphas[0])
            base, tilt = linear_parts(flux, cons, [xmask_ref[here, :] > 0.0 for here in at], LAMBDA[0])
            for i, here in enumerate(at):
                x_part = base[i] + alphas[0] * tilt[i] + xmask_ref[here, :] * (bent[i + 1] - bent[i])
                change = x_part + acc_y[here, :] + spread[here]
                register = REGISTER_DECAY * reg_ref[v, here, :] - change
                reg_out[v, here, :] = register
                state_out[v, here, :] = state_ref[v, here, :] + UPDATE_WEIGHT * register
        for copy in copies(v):
            copy.start()
        return carry

    lax.fori_loop(0, NV, per_var, 0)
    for v in range(NV):
        for copy in copies(v):
            copy.wait()


def f32(*shape):
    return jax.ShapeDtypeStruct(shape, jnp.float32)


def near(*shape):
    return pltpu.VMEM(shape, jnp.float32)


ROOM = pltpu.CompilerParams(vmem_limit_bytes=16 * 1024 * 1024)


def held(value):
    return pltpu.with_memory_space_constraint(value, pltpu.VMEM)


def afar(value):
    return pltpu.with_memory_space_constraint(value, pltpu.HBM)


def advance(state, register, top_ghost, flags):
    flat = state.reshape(NV, ROWS, CZ)
    halves, n_z = lax.axis_size("gx_0"), lax.axis_size("gz")
    n_plane = lax.axis_size("gx_1") * lax.axis_size("gx_2") * lax.axis_size("gx_3")
    n_x = halves * n_plane

    far = pl.BlockSpec(memory_space=pltpu.HBM)
    close = pl.BlockSpec(memory_space=pltpu.VMEM)
    planes, strips = (NV, LONG, SUB, CZ), (NV, CY, SUB, CZ)
    near_state, own = pl.pallas_call(
        open_kernel,
        in_specs=[far],
        out_shape=(near(NV, ROWS, CZ), near(halves * n_z, NV * HALO + 1, CZ)),
        scratch_shapes=[pltpu.SemaphoreType.DMA((NV,))],
        compiler_params=ROOM, name="open",
    )(afar(flat))
    by_line = lax.all_to_all(held(own), ZLINE, 0, 0, tiled=True)
    yu, ybase, ytilt, xmask, zmask = pl.pallas_call(
        prepare_kernel,
        out_shape=(
            near(*planes), near(*strips), near(*strips), near(ROWS, CZ), near(SUB, ROWS),
        ),
        scratch_shapes=[pltpu.VMEM(planes, jnp.float32)],
        compiler_params=ROOM, name="prepare",
    )(held(near_state), top_ghost.transpose(0, 2, 1, 3), flags.transpose(0, 2, 1))
    relayed = pl.pallas_call(relay_kernel, out_shape=near(n_plane, 1, CZ), compiler_params=ROOM, name="relay")(held(by_line))
    speeds = lax.all_to_all(held(relayed), PLANE, 0, 0, tiled=True)
    zu, zbase, ztilt = pl.pallas_call(
        z_kernel,
        out_shape=(near(*planes), near(*strips), near(*strips)),
        scratch_shapes=[pltpu.VMEM(planes, jnp.float32), pltpu.VMEM((NV, CZ + 8, ROWS), jnp.float32)],
        compiler_params=ROOM, name="z_prepare",
    )(held(by_line), held(near_state), held(zmask))

    ring = [(i, (i + 1) % n_x) for i in range(n_x)]
    seam = [pair for pair in ring if pair[0] % n_plane == n_plane - 1]
    rest = [pair for pair in ring if pair not in seam]

    def back(pairs):
        return [(b, a) for a, b in pairs]

    blocks = near_state.reshape(state.shape)
    upper, lower = blocks[:, CX - HALO :], blocks[:, :HALO]
    xlo_seam = lax.ppermute(upper, GX, seam)
    xhi_seam = lax.ppermute(lower, GX, back(seam))
    xlo = lax.ppermute(upper, GX, rest)
    xhi = lax.ppermute(lower, GX, back(rest))

    new_state, new_register = pl.pallas_call(
        step_kernel,
        out_shape=(f32(NV, ROWS, CZ), f32(NV, ROWS, CZ)),
        in_specs=[close] * 14 + [far],
        out_specs=(far, far),
        scratch_shapes=[
            pltpu.VMEM((CY, CX, CZ), jnp.float32),
            pltpu.VMEM((NV, ROWS, CZ), jnp.float32),
            pltpu.VMEM(planes, jnp.float32),
            pltpu.VMEM(planes, jnp.float32),
            pltpu.VMEM((NV, 2 * HALO, CY, CZ), jnp.float32),
            pltpu.VMEM((NV, 2 * HALO, CY, CZ), jnp.float32),
            pltpu.VMEM((ROWS, CZ), jnp.float32),
            pltpu.VMEM((CZ, ROWS), jnp.float32),
            pltpu.VMEM((NV, ROWS, CZ), jnp.float32),
            pltpu.VMEM((NV, ROWS, CZ), jnp.float32),
            pltpu.VMEM((NV, ROWS, CZ), jnp.float32),
            pltpu.SemaphoreType.DMA((3, NV)),
        ],
        compiler_params=ROOM, name="step",
    )(
        *map(held, (
            speeds, near_state, xlo, xhi, xlo_seam, xhi_seam,
            yu, ybase, ytilt, zu, zbase, ztilt, xmask, zmask,
        )),
        afar(register.reshape(NV, ROWS, CZ)),
    )
    return (new_state.reshape(state.shape), new_register.reshape(state.shape))


def solution(mesh):
    finer = Mesh(
        mesh.devices.reshape(2, 8, 4, 2, mesh.shape["gz"]), ("gx_0", "gx_1", "gx_2", "gx_3", "gz")
    )
    placed = P(None, GX, None, "gz")
    return jax.shard_map(
        advance,
        mesh=finer,
        in_specs=(placed, placed, placed, P(GX, None, "gz")),
        out_specs=(placed, placed),
        check_vma=False,
    )
```

```python
import jax
import jax.numpy as jnp
from jax import lax
from jax.experimental import pallas as pl
from jax.experimental.pallas import tpu as pltpu
from jax.sharding import Mesh
from jax.sharding import PartitionSpec as P

GX = ("gx_0", "gx_1", "gx_2", "gx_3")
PLANE = ("gx_1", "gx_2", "gx_3")
ZLINE = ("gx_0", "gz")

GAMMA = 1.4
EPS_WENO = 1e-06
LAMBDA = (0.1, 0.15, 0.1)
REGISTER_DECAY = -5.0 / 9.0
UPDATE_WEIGHT = 15.0 / 16.0

NV = 5
CX = 8
CY = 16
CZ = 128
ROWS = CX * CY
HALO = 3
SUB = 8
LONG = 16 + 2 * HALO


def primitives(cons):
    inverse = 1.0 / cons[0]
    vels = [cons[k] * inverse for k in (1, 2, 3)]
    kinetic = cons[1] * vels[0] + cons[2] * vels[1] + cons[3] * vels[2]
    pressure = (GAMMA - 1.0) * (cons[4] - 0.5 * kinetic)
    return inverse, vels, pressure


def fetch(pairs, sems):
    copies = [pltpu.make_async_copy(src, dst, sems.at[i]) for i, (src, dst) in enumerate(pairs)]
    for copy in copies:
        copy.start()
    for copy in copies:
        copy.wait()


def line_neighbours():
    n_z, here = lax.axis_size("gz"), lax.axis_index("gz")
    first = lax.axis_index("gx_0") * n_z
    return first + lax.rem(here + n_z - 1, n_z), first + lax.rem(here + 1, n_z)


def open_kernel(far_ref, state_ref, out_ref, sems):
    fetch([(far_ref.at[v], state_ref.at[v]) for v in range(NV)], sems)
    best = [None] * 3
    for block in range(ROWS // SUB):
        rows = slice(block * SUB, block * SUB + SUB)
        inverse, vels, pressure = primitives([state_ref[v, rows, :] for v in range(NV)])
        sound = jnp.sqrt(GAMMA * pressure * inverse)
        for k in range(3):
            speed = jnp.abs(vels[k]) + sound
            best[k] = speed if block == 0 else jnp.maximum(best[k], speed)
    lane = lax.broadcasted_iota(jnp.int32, (1, CZ), 1)
    packed = jnp.zeros((1, CZ), jnp.float32)
    for k in range(3):
        top = jnp.max(jnp.max(best[k], axis=0, keepdims=True), axis=1, keepdims=True)
        packed = jnp.where(lane == k, top, packed)
    firsts, lasts = [], []
    for v in range(NV):
        turned = state_ref[v].T
        firsts.append(turned[:HALO])
        lasts.append(turned[CZ - HALO :])
    _, after = line_neighbours()
    for to in range(out_ref.shape[0]):
        forward = after == to
        for v in range(NV):
            out_ref[to, v * HALO : v * HALO + HALO, :] = jnp.where(forward, lasts[v], firsts[v])
        out_ref[to, NV * HALO : NV * HALO + 1, :] = packed


def relay_kernel(got_ref, out_ref):
    row = slice(NV * HALO, NV * HALO + 1)
    best = got_ref[0, row, :]
    for i in range(1, got_ref.shape[0]):
        best = jnp.maximum(best, got_ref[i, row, :])
    for to in range(out_ref.shape[0]):
        out_ref[to] = best


def flux_of(cons, var):
    _, vels, pressure = primitives(cons)
    velocity = vels[var - 1]
    flux = [(cons[v] + pressure if v == 4 else cons[v]) * velocity for v in range(NV)]
    flux[var] = flux[var] + pressure
    return flux


def linear_parts(flux, cons, masks, scale):
    count = len(flux) - 2 * HALO

    def face(j):
        inner, outer = flux[j + 2] + flux[j + 3], flux[j + 1] + flux[j + 4]
        central = 37.0 * inner - 8.0 * outer + (flux[j] + flux[j + 5])
        return central, 7.0 * inner - outer, (cons[j + 4] - cons[j + 1]) - 3.0 * (cons[j + 3] - cons[j + 2])

    faces = [face(j) for j in range(count + 1)]
    base, tilt = [], []
    for low, high, mask in zip(faces, faces[1:], masks):
        base.append(jnp.where(mask, (scale / 12.0) * (high[1] - low[1]), (scale / 60.0) * (high[0] - low[0])))
        tilt.append(jnp.where(mask, (scale / 12.0) * (high[2] - low[2]), 0.0))
    return base, tilt


EPS_SCALED = 16.0 * EPS_WENO
CURVE = 13.0 / 3.0


def bent_faces(flux, cons, alpha):
    count = len(flux) - 2 * HALO + 1
    moved = [alpha * u for u in cons]

    def slopes(vals):
        step = [b - a for a, b in zip(vals, vals[1:])]
        bend = [None] + [b - a for a, b in zip(step, step[1:])]
        turn = [None] + [b - a for a, b in zip(bend[1:], bend[2:])]
        base = [None] + [CURVE * (d * d) + EPS_SCALED for d in bend[1:]]
        return step, bend, turn, base

    def pull(beta_a, beta_b, beta_c, near_turn, far_turn):
        u, w = beta_b / beta_a, beta_b / beta_c
        u, w = u * u, w * w
        w = 3.0 * w
        return ((u + u) * near_turn + w * far_turn) / (6.0 + u + w)

    pe, pd, pt, pk = slopes([f + m for f, m in zip(flux, moved)])
    me, md, mt, mk = slopes([f - m for f, m in zip(flux, moved)])
    out = []
    for j in range(count):
        bc, cd = pe[j + 1], pe[j + 2]
        ta, tb, tc = pd[j + 1] + (bc + bc), bc + cd, pd[j + 3] - (cd + cd)
        plus = pull(pk[j + 1] + ta * ta, pk[j + 2] + tb * tb, pk[j + 3] + tc * tc, pt[j + 1], pt[j + 2])
        bc, cd = me[j + 3], me[j + 2]
        ta, tb, tc = md[j + 4] - (bc + bc), bc + cd, md[j + 2] + (cd + cd)
        minus = pull(mk[j + 4] + ta * ta, mk[j + 3] + tb * tb, mk[j + 2] + tc * tc, mt[j + 3], mt[j + 2])
        out.append(minus - plus)
    return out


def prepare_kernel(
    state_ref, top_ref, flag_ref, yu_ref, ybase_ref, ytilt_ref, xmask_ref, zmask_ref, yf_ref
):
    square = (CY, CY)
    diagonal = lax.broadcasted_iota(jnp.int32, square, 0) == lax.broadcasted_iota(jnp.int32, square, 1)
    for x in range(CX):
        spread = jnp.broadcast_to(flag_ref[x].astype(jnp.float32), square)
        column = jnp.max(jnp.where(diagonal, spread, 0.0), axis=1, keepdims=True)
        xmask_ref[x * CY : x * CY + CY, :] = jnp.broadcast_to(column, (CY, CZ)) * (LAMBDA[0] / 12.0)
    zmask_ref[...] = xmask_ref[...].T[:SUB] * (LAMBDA[2] / LAMBDA[0])

    def y_store(to, cons):
        flux = flux_of(cons, 2)
        for v in range(NV):
            yf_ref[v, to] = flux[v]
            yu_ref[v, to] = cons[v]

    for i in range(CY):
        cons = [state_ref[v, pl.ds(i, CX, stride=CY), :] for v in range(NV)]
        y_store(i + HALO, cons)
        if i < HALO:
            y_store(HALO - 1 - i, [-c if v == 2 else c for v, c in enumerate(cons)])
            y_store(HALO + CY + i, [top_ref[v, i] for v in range(NV)])

    masks = [xmask_ref[pl.ds(i, CX, stride=CY), :] > 0.0 for i in range(CY)]

    def per_var(v, carry):
        planes = range(LONG)
        base, tilt = linear_parts([yf_ref[v, i] for i in planes], [yu_ref[v, i] for i in planes], masks, LAMBDA[1])
        for i in range(CY):
            ybase_ref[v, i] = base[i]
            ytilt_ref[v, i] = tilt[i]
        return carry

    lax.fori_loop(0, NV, per_var, 0)


def z_kernel(got_ref, state_ref, zmask_ref, zu_ref, zbase_ref, ztilt_ref, zf_ref, line):
    before, after = line_neighbours()
    for v in range(NV):
        rows = slice(v * HALO, v * HALO + HALO)
        line[v, :HALO, :] = got_ref[before, rows, :]
        line[v, HALO : HALO + CZ, :] = state_ref[v].T
        line[v, HALO + CZ : 2 * HALO + CZ, :] = got_ref[after, rows, :]
    for i in range(LONG):
        cons = [line[v, pl.ds(i, SUB, stride=CZ // SUB), :] for v in range(NV)]
        flux = flux_of(cons, 3)
        for v in range(NV):
            zf_ref[v, i] = flux[v]
            zu_ref[v, i] = cons[v]
    mask = zmask_ref[...] > 0.0

    def per_var(v, carry):
        planes = range(LONG)
        base, tilt = linear_parts(
            [zf_ref[v, i] for i in planes], [zu_ref[v, i] for i in planes], [mask] * CY, LAMBDA[2]
        )
        for i in range(CY):
            zbase_ref[v, i] = base[i]
            ztilt_ref[v, i] = tilt[i]
        return carry

    lax.fori_loop(0, NV, per_var, 0)


def step_kernel(
    speed_ref, state_ref, xlo_ref, xhi_ref, xlo_seam_ref, xhi_seam_ref,
    yu_ref, ybase_ref, ytilt_ref, zu_ref, zbase_ref, ztilt_ref, xmask_ref, zmask_ref, old_reg_ref,
    far_state_ref, far_reg_ref,
    ymask_ref, xf_ref, yf_ref, zf_ref, side_f, side_u, acc_y, acc_z, reg_ref, state_out, reg_out, sems,
):
    loads = [pltpu.make_async_copy(old_reg_ref.at[v], reg_ref.at[v], sems.at[2, v]) for v in range(NV)]
    for load in loads:
        load.start()

    best = speed_ref[0]
    for i in range(1, speed_ref.shape[0]):
        best = jnp.maximum(best, speed_ref[i])
    lane = lax.broadcasted_iota(jnp.int32, (1, CZ), 1)
    alphas = [jnp.max(jnp.where(lane == k, best, 0.0), axis=1, keepdims=True) for k in range(3)]
    halves = [slice(h * SUB, h * SUB + SUB) for h in range(CY // SUB)]

    for i in range(HALO):
        for rows in halves:
            for at, rest, seam in ((i, xlo_ref, xlo_seam_ref), (HALO + i, xhi_ref, xhi_seam_ref)):
                cons = [rest[v, i, rows, :] + seam[v, i, rows, :] for v in range(NV)]
                flux = flux_of(cons, 1)
                for v in range(NV):
                    side_f[v, at, rows, :] = flux[v]
                    side_u[v, at, rows, :] = cons[v]

    for i in range(LONG):
        for cons_ref, flux_ref, var in ((yu_ref, yf_ref, 2), (zu_ref, zf_ref, 3)):
            flux = flux_of([cons_ref[v, i] for v in range(NV)], var)
            for v in range(NV):
                flux_ref[v, i] = flux[v]
    for block in range(ROWS // SUB):
        rows = slice(block * SUB, block * SUB + SUB)
        flux = flux_of([state_ref[v, rows, :] for v in range(NV)], 1)
        for v in range(NV):
            xf_ref[v, rows, :] = flux[v]
    for y in range(CY):
        ymask_ref[y] = xmask_ref[pl.ds(y, CX, stride=CY), :] * (LAMBDA[1] / LAMBDA[0])
    for load in loads:
        load.wait()

    def copies(v):
        return [
            pltpu.make_async_copy(state_out.at[v], far_state_ref.at[v], sems.at[0, v]),
            pltpu.make_async_copy(reg_out.at[v], far_reg_ref.at[v], sems.at[1, v]),
        ]

    def per_var(v, carry):
        bent = bent_faces([zf_ref[v, i] for i in range(LONG)], [zu_ref[v, i] for i in range(LONG)], alphas[2])
        for i in range(CY):
            acc_z[pl.ds(i, SUB, stride=CZ // SUB), :] = (
                zbase_ref[v, i] + alphas[2] * ztilt_ref[v, i] + zmask_ref[...] * (bent[i + 1] - bent[i])
            )
        bent = bent_faces([yf_ref[v, i] for i in range(LONG)], [yu_ref[v, i] for i in range(LONG)], alphas[1])
        for i in range(CY):
            acc_y[pl.ds(i, CX, stride=CY), :] = (
                ybase_ref[v, i] + alphas[1] * ytilt_ref[v, i] + ymask_ref[i] * (bent[i + 1] - bent[i])
            )
        spread = acc_z[...].T
        for rows in halves:
            at = [slice(i * CY + rows.start, i * CY + rows.stop) for i in range(CX)]
            flux = (
                [side_f[v, i, rows, :] for i in range(HALO)]
                + [xf_ref[v, here, :] for here in at]
                + [side_f[v, HALO + i, rows, :] for i in range(HALO)]
            )
            cons = (
                [side_u[v, i, rows, :] for i in range(HALO)]
                + [state_ref[v, here, :] for here in at]
                + [side_u[v, HALO + i, rows, :] for i in range(HALO)]
            )
            bent = bent_faces(flux, cons, alphas[0])
            base, tilt = linear_parts(flux, cons, [xmask_ref[here, :] > 0.0 for here in at], LAMBDA[0])
            for i, here in enumerate(at):
                x_part = base[i] + alphas[0] * tilt[i] + xmask_ref[here, :] * (bent[i + 1] - bent[i])
                change = x_part + acc_y[here, :] + spread[here]
                register = REGISTER_DECAY * reg_ref[v, here, :] - change
                reg_out[v, here, :] = register
                state_out[v, here, :] = state_ref[v, here, :] + UPDATE_WEIGHT * register
        for copy in copies(v):
            copy.start()
        return carry

    lax.fori_loop(0, NV, per_var, 0)
    for v in range(NV):
        for copy in copies(v):
            copy.wait()


def f32(*shape):
    return jax.ShapeDtypeStruct(shape, jnp.float32)


def near(*shape):
    return pltpu.VMEM(shape, jnp.float32)


ROOM = pltpu.CompilerParams(vmem_limit_bytes=16 * 1024 * 1024)


def held(value):
    return pltpu.with_memory_space_constraint(value, pltpu.VMEM)


def afar(value):
    return pltpu.with_memory_space_constraint(value, pltpu.HBM)


def advance(state, register, top_ghost, flags):
    flat = state.reshape(NV, ROWS, CZ)
    halves, n_z = lax.axis_size("gx_0"), lax.axis_size("gz")
    n_plane = lax.axis_size("gx_1") * lax.axis_size("gx_2") * lax.axis_size("gx_3")

    far = pl.BlockSpec(memory_space=pltpu.HBM)
    close = pl.BlockSpec(memory_space=pltpu.VMEM)
    planes, strips = (NV, LONG, SUB, CZ), (NV, CY, SUB, CZ)
    near_state, own = pl.pallas_call(
        open_kernel,
        in_specs=[far],
        out_shape=(near(NV, ROWS, CZ), near(halves * n_z, NV * HALO + 1, CZ)),
        scratch_shapes=[pltpu.SemaphoreType.DMA((NV,))],
        compiler_params=ROOM, name="open",
    )(afar(flat))
    by_line = lax.all_to_all(held(own), ZLINE, 0, 0, tiled=True)
    yu, ybase, ytilt, xmask, zmask = pl.pallas_call(
        prepare_kernel,
        out_shape=(
            near(*planes), near(*strips), near(*strips), near(ROWS, CZ), near(SUB, ROWS),
        ),
        scratch_shapes=[pltpu.VMEM(planes, jnp.float32)],
        compiler_params=ROOM, name="prepare",
    )(held(near_state), top_ghost.transpose(0, 2, 1, 3), flags.transpose(0, 2, 1))
    relayed = pl.pallas_call(relay_kernel, out_shape=near(n_plane, 1, CZ), compiler_params=ROOM, name="relay")(held(by_line))
    speeds = lax.all_to_all(held(relayed), PLANE, 0, 0, tiled=True)
    zu, zbase, ztilt = pl.pallas_call(
        z_kernel,
        out_shape=(near(*planes), near(*strips), near(*strips)),
        scratch_shapes=[pltpu.VMEM(planes, jnp.float32), pltpu.VMEM((NV, CZ + 8, ROWS), jnp.float32)],
        compiler_params=ROOM, name="z_prepare",
    )(held(by_line), held(near_state), held(zmask))

    ahead = [(i, i + 1) for i in range(n_plane - 1)]
    lows = [((h + 1) % halves * n_plane, h * n_plane) for h in range(halves)]
    highs = [(h * n_plane + n_plane - 1, (h + 1) % halves * n_plane + n_plane - 1) for h in range(halves)]

    blocks = near_state.reshape(state.shape)
    upper, lower = blocks[:, CX - HALO :], blocks[:, :HALO]
    xhi = lax.ppermute(lower, PLANE, [(b, a) for a, b in ahead])
    low_end = lax.ppermute(lower, GX, lows)
    high_end = lax.ppermute(upper, GX, highs)
    xlo = lax.ppermute(upper, PLANE, ahead)
    xhi_seam = lax.ppermute(low_end, PLANE, [(0, n_plane - 1)])
    xlo_seam = lax.ppermute(high_end, PLANE, [(n_plane - 1, 0)])

    new_state, new_register = pl.pallas_call(
        step_kernel,
        out_shape=(f32(NV, ROWS, CZ), f32(NV, ROWS, CZ)),
        in_specs=[close] * 14 + [far],
        out_specs=(far, far),
        scratch_shapes=[
            pltpu.VMEM((CY, CX, CZ), jnp.float32),
            pltpu.VMEM((NV, ROWS, CZ), jnp.float32),
            pltpu.VMEM(planes, jnp.float32),
            pltpu.VMEM(planes, jnp.float32),
            pltpu.VMEM((NV, 2 * HALO, CY, CZ), jnp.float32),
            pltpu.VMEM((NV, 2 * HALO, CY, CZ), jnp.float32),
            pltpu.VMEM((ROWS, CZ), jnp.float32),
            pltpu.VMEM((CZ, ROWS), jnp.float32),
            pltpu.VMEM((NV, ROWS, CZ), jnp.float32),
            pltpu.VMEM((NV, ROWS, CZ), jnp.float32),
            pltpu.VMEM((NV, ROWS, CZ), jnp.float32),
            pltpu.SemaphoreType.DMA((3, NV)),
        ],
        compiler_params=ROOM, name="step",
    )(
        *map(held, (
            speeds, near_state, xlo, xhi, xlo_seam, xhi_seam,
            yu, ybase, ytilt, zu, zbase, ztilt, xmask, zmask,
        )),
        afar(register.reshape(NV, ROWS, CZ)),
    )
    return (new_state.reshape(state.shape), new_register.reshape(state.shape))


def solution(mesh):
    finer = Mesh(
        mesh.devices.reshape(2, 8, 4, 2, mesh.shape["gz"]), ("gx_0", "gx_1", "gx_2", "gx_3", "gz")
    )
    placed = P(None, GX, None, "gz")
    return jax.shard_map(
        advance,
        mesh=finer,
        in_specs=(placed, placed, placed, P(GX, None, "gz")),
        out_specs=(placed, placed),
        check_vma=False,
    )
```

```python
import jax
import jax.numpy as jnp
from jax import lax
from jax.experimental import pallas as pl
from jax.experimental.pallas import tpu as pltpu
from jax.sharding import Mesh
from jax.sharding import PartitionSpec as P

GX = ("gx_0", "gx_1", "gx_2", "gx_3")
PLANE = ("gx_1", "gx_2", "gx_3")
ZLINE = ("gx_0", "gz")

GAMMA = 1.4
EPS_WENO = 1e-06
LAMBDA = (0.1, 0.15, 0.1)
REGISTER_DECAY = -5.0 / 9.0
UPDATE_WEIGHT = 15.0 / 16.0

NV = 5
CX = 8
CY = 16
CZ = 128
ROWS = CX * CY
HALO = 3
SUB = 8
LONG = 16 + 2 * HALO


def primitives(cons):
    inverse = 1.0 / cons[0]
    vels = [cons[k] * inverse for k in (1, 2, 3)]
    kinetic = cons[1] * vels[0] + cons[2] * vels[1] + cons[3] * vels[2]
    pressure = (GAMMA - 1.0) * (cons[4] - 0.5 * kinetic)
    return inverse, vels, pressure


def fetch(pairs, sems):
    copies = [pltpu.make_async_copy(src, dst, sems.at[i]) for i, (src, dst) in enumerate(pairs)]
    for copy in copies:
        copy.start()
    for copy in copies:
        copy.wait()


def line_neighbours():
    n_z, here = lax.axis_size("gz"), lax.axis_index("gz")
    first = lax.axis_index("gx_0") * n_z
    return first + lax.rem(here + n_z - 1, n_z), first + lax.rem(here + 1, n_z)


def open_kernel(
    far_ref, far_top_ref, far_flag_ref, state_ref, out_ref, ends_ref, top_ref, flag_ref, sems
):
    pairs = [(far_ref.at[v], state_ref.at[v]) for v in range(NV)]
    fetch(pairs + [(far_top_ref, top_ref), (far_flag_ref, flag_ref)], sems)
    best = [None] * 3
    for block in range(ROWS // SUB):
        rows = slice(block * SUB, block * SUB + SUB)
        inverse, vels, pressure = primitives([state_ref[v, rows, :] for v in range(NV)])
        sound = jnp.sqrt(GAMMA * pressure * inverse)
        for k in range(3):
            speed = jnp.abs(vels[k]) + sound
            best[k] = speed if block == 0 else jnp.maximum(best[k], speed)
    lane = lax.broadcasted_iota(jnp.int32, (1, CZ), 1)
    packed = jnp.zeros((1, CZ), jnp.float32)
    for k in range(3):
        top = jnp.max(jnp.max(best[k], axis=0, keepdims=True), axis=1, keepdims=True)
        packed = jnp.where(lane == k, top, packed)
    firsts, lasts = [], []
    for v in range(NV):
        turned = state_ref[v].T
        firsts.append(turned[:HALO])
        lasts.append(turned[CZ - HALO :])
    _, after = line_neighbours()
    for to in range(out_ref.shape[0]):
        forward = after == to
        for v in range(NV):
            out_ref[to, v * HALO : v * HALO + HALO, :] = jnp.where(forward, lasts[v], firsts[v])
        out_ref[to, NV * HALO : NV * HALO + 1, :] = packed
    first = plane_place()[0] == 0
    for v in range(NV):
        for i in range(HALO):
            for h in range(CY // SUB):
                low, high = i * CY + h * SUB, (CX - HALO + i) * CY + h * SUB
                ends_ref[v, i, h * SUB : h * SUB + SUB, :] = jnp.where(
                    first, state_ref[v, low : low + SUB, :], state_ref[v, high : high + SUB, :]
                )


def plane_place():
    place, last = 0, 1
    for axis in PLANE:
        place = place * lax.axis_size(axis) + lax.axis_index(axis)
        last = last * lax.axis_size(axis)
    return place, last - 1


def relay_kernel(got_ref, out_ref):
    row = slice(NV * HALO, NV * HALO + 1)
    best = got_ref[0, row, :]
    for i in range(1, got_ref.shape[0]):
        best = jnp.maximum(best, got_ref[i, row, :])
    for to in range(out_ref.shape[0]):
        out_ref[to] = best


def peak_kernel(speed_ref, out_ref):
    best = speed_ref[0]
    for i in range(1, speed_ref.shape[0]):
        best = jnp.maximum(best, speed_ref[i])
    lane = lax.broadcasted_iota(jnp.int32, (1, CZ), 1)
    for k in range(3):
        top = jnp.max(jnp.where(lane == k, best, 0.0), axis=1, keepdims=True)
        out_ref[k] = jnp.broadcast_to(top, (SUB, CZ))


def flux_of(cons, var):
    _, vels, pressure = primitives(cons)
    velocity = vels[var - 1]
    flux = [(cons[v] + pressure if v == 4 else cons[v]) * velocity for v in range(NV)]
    flux[var] = flux[var] + pressure
    return flux


def linear_parts(flux, cons, masks, scale):
    count = len(flux) - 2 * HALO

    def face(j):
        inner, outer = flux[j + 2] + flux[j + 3], flux[j + 1] + flux[j + 4]
        central = 37.0 * inner - 8.0 * outer + (flux[j] + flux[j + 5])
        return central, 7.0 * inner - outer, (cons[j + 4] - cons[j + 1]) - 3.0 * (cons[j + 3] - cons[j + 2])

    faces = [face(j) for j in range(count + 1)]
    base, tilt = [], []
    for low, high, mask in zip(faces, faces[1:], masks):
        base.append(jnp.where(mask, (scale / 12.0) * (high[1] - low[1]), (scale / 60.0) * (high[0] - low[0])))
        tilt.append(jnp.where(mask, (scale / 12.0) * (high[2] - low[2]), 0.0))
    return base, tilt


EPS_SCALED = 4.0 * EPS_WENO
CURVE = 4.0 / 3.0


def bent_faces(flux, cons, alpha):
    count = len(flux) - 2 * HALO + 1
    moved = [alpha * u for u in cons]

    def slopes(vals):
        step = [b - a for a, b in zip(vals, vals[1:])]
        bend = [None] + [b - a for a, b in zip(step, step[1:])]
        turn = [None] + [b - a for a, b in zip(bend[1:], bend[2:])]
        base = [None] + [CURVE * (d * d) + EPS_SCALED for d in bend[1:]]
        return step, bend, turn, base

    def pull(beta_a, beta_b, beta_c, near_turn, far_turn):
        u, w = beta_b / beta_a, beta_b / beta_c
        u, w = u * u, w * w
        w = 3.0 * w
        return ((u + u) * near_turn + w * far_turn) / (6.0 + u + w)

    pe, pd, pt, pk = slopes([f + m for f, m in zip(flux, moved)])
    me, md, mt, mk = slopes([f - m for f, m in zip(flux, moved)])
    out = []
    for j in range(count):
        bc, cd = pe[j + 1], pe[j + 2]
        plus = pull(
            pk[j + 1] + bc * (bc + pd[j + 1]), pk[j + 2] + bc * cd, pk[j + 3] + cd * (cd - pd[j + 3]), pt[j + 1], pt[j + 2]
        )
        bc, cd = me[j + 3], me[j + 2]
        minus = pull(
            mk[j + 4] + bc * (bc - md[j + 4]), mk[j + 3] + bc * cd, mk[j + 2] + cd * (cd + md[j + 2]), mt[j + 3], mt[j + 2]
        )
        out.append(minus - plus)
    return out


def step_kernel(
    speed_ref, state_ref, xlo_ref, xhi_ref, seam_ref, helped_ref, got_ref, top_ref, flag_ref, old_reg_ref,
    far_state_ref, far_reg_ref,
    xmask_ref, ymask_ref, xf_ref, yf_ref, yu_ref, zf_ref, zu_ref, line, side_f, side_u, acc_y, acc_z,
    reg_ref, state_out, reg_out, sems,
):
    def load(v):
        return pltpu.make_async_copy(old_reg_ref.at[v], reg_ref.at[v], sems.at[2, v])

    for v in range(NV):
        load(v).start()

    square = (CY, CY)
    diagonal = lax.broadcasted_iota(jnp.int32, square, 0) == lax.broadcasted_iota(jnp.int32, square, 1)
    for x in range(CX):
        spread = jnp.broadcast_to(flag_ref[x].astype(jnp.float32), square)
        column = jnp.max(jnp.where(diagonal, spread, 0.0), axis=1, keepdims=True)
        xmask_ref[x * CY : x * CY + CY, :] = jnp.broadcast_to(column, (CY, CZ)) * (LAMBDA[0] / 12.0)
    for y in range(CY):
        ymask_ref[y] = xmask_ref[pl.ds(y, CX, stride=CY), :] * (LAMBDA[1] / LAMBDA[0])
    zmask = xmask_ref[...].T[:SUB] * (LAMBDA[2] / LAMBDA[0])

    before, after = line_neighbours()
    for v in range(NV):
        rows = slice(v * HALO, v * HALO + HALO)
        line[v, :HALO, :] = got_ref[before, rows, :]
        line[v, HALO : HALO + CZ, :] = state_ref[v].T
        line[v, HALO + CZ : 2 * HALO + CZ, :] = got_ref[after, rows, :]

    def keep(to, cons, var, flux_ref, cons_ref):
        flux = flux_of(cons, var)
        for v in range(NV):
            flux_ref[v, to] = flux[v]
            cons_ref[v, to] = cons[v]

    for i in range(LONG):
        keep(i, [line[v, pl.ds(i, SUB, stride=CZ // SUB), :] for v in range(NV)], 3, zf_ref, zu_ref)
    for i in range(CY):
        cons = [state_ref[v, pl.ds(i, CX, stride=CY), :] for v in range(NV)]
        keep(i + HALO, cons, 2, yf_ref, yu_ref)
        if i < HALO:
            keep(HALO - 1 - i, [-c if v == 2 else c for v, c in enumerate(cons)], 2, yf_ref, yu_ref)
            keep(HALO + CY + i, [top_ref[v, i] for v in range(NV)], 2, yf_ref, yu_ref)

    alphas = [speed_ref[k] for k in range(3)]
    halves = [slice(h * SUB, h * SUB + SUB) for h in range(CY // SUB)]

    place, last = plane_place()
    for i in range(HALO):
        for rows in halves:
            for at, side_ref, end in ((i, xlo_ref, 0), (HALO + i, xhi_ref, last)):
                cons = [
                    jnp.where(
                        place == end, seam_ref[v, i, rows, :] + helped_ref[v, i, rows, :], side_ref[v, i, rows, :]
                    )
                    for v in range(NV)
                ]
                flux = flux_of(cons, 1)
                for v in range(NV):
                    side_f[v, at, rows, :] = flux[v]
                    side_u[v, at, rows, :] = cons[v]

    for block in range(ROWS // SUB):
        rows = slice(block * SUB, block * SUB + SUB)
        flux = flux_of([state_ref[v, rows, :] for v in range(NV)], 1)
        for v in range(NV):
            xf_ref[v, rows, :] = flux[v]

    def copies(v):
        return [
            pltpu.make_async_copy(state_out.at[v], far_state_ref.at[v], sems.at[0, v]),
            pltpu.make_async_copy(reg_out.at[v], far_reg_ref.at[v], sems.at[1, v]),
        ]

    def per_var(v, carry):
        flux, cons = [zf_ref[v, i] for i in range(LONG)], [zu_ref[v, i] for i in range(LONG)]
        bent = bent_faces(flux, cons, alphas[2])
        base, tilt = linear_parts(flux, cons, [zmask > 0.0] * CY, LAMBDA[2])
        for i in range(CY):
            acc_z[pl.ds(i, SUB, stride=CZ // SUB), :] = (
                base[i] + alphas[2] * tilt[i] + zmask * (bent[i + 1] - bent[i])
            )
        flux, cons = [yf_ref[v, i] for i in range(LONG)], [yu_ref[v, i] for i in range(LONG)]
        bent = bent_faces(flux, cons, alphas[1])
        base, tilt = linear_parts(flux, cons, [ymask_ref[i] > 0.0 for i in range(CY)], LAMBDA[1])
        for i in range(CY):
            acc_y[pl.ds(i, CX, stride=CY), :] = (
                base[i] + alphas[1] * tilt[i] + ymask_ref[i] * (bent[i + 1] - bent[i])
            )
        spread = acc_z[...].T
        load(v).wait()
        for rows in halves:
            at = [slice(i * CY + rows.start, i * CY + rows.stop) for i in range(CX)]
            flux = (
                [side_f[v, i, rows, :] for i in range(HALO)]
                + [xf_ref[v, here, :] for here in at]
                + [side_f[v, HALO + i, rows, :] for i in range(HALO)]
            )
            cons = (
                [side_u[v, i, rows, :] for i in range(HALO)]
                + [state_ref[v, here, :] for here in at]
                + [side_u[v, HALO + i, rows, :] for i in range(HALO)]
            )
            bent = bent_faces(flux, cons, alphas[0])
            base, tilt = linear_parts(flux, cons, [xmask_ref[here, :] > 0.0 for here in at], LAMBDA[0])
            for i, here in enumerate(at):
                x_part = base[i] + alphas[0] * tilt[i] + xmask_ref[here, :] * (bent[i + 1] - bent[i])
                change = x_part + acc_y[here, :] + spread[here]
                register = REGISTER_DECAY * reg_ref[v, here, :] - change
                reg_out[v, here, :] = register
                state_out[v, here, :] = state_ref[v, here, :] + UPDATE_WEIGHT * register
        for copy in copies(v):
            copy.start()
        return carry

    lax.fori_loop(0, NV, per_var, 0)
    for v in range(NV):
        for copy in copies(v):
            copy.wait()


def f32(*shape):
    return jax.ShapeDtypeStruct(shape, jnp.float32)


def near(*shape):
    return pltpu.VMEM(shape, jnp.float32)


ROOM = pltpu.CompilerParams(vmem_limit_bytes=16 * 1024 * 1024)


def held(value):
    return pltpu.with_memory_space_constraint(value, pltpu.VMEM)


def afar(value):
    return pltpu.with_memory_space_constraint(value, pltpu.HBM)


def advance(state, register, top_ghost, flags):
    flat = state.reshape(NV, ROWS, CZ)
    halves, n_z = lax.axis_size("gx_0"), lax.axis_size("gz")
    n_plane = lax.axis_size("gx_1") * lax.axis_size("gx_2") * lax.axis_size("gx_3")

    far = pl.BlockSpec(memory_space=pltpu.HBM)
    close = pl.BlockSpec(memory_space=pltpu.VMEM)
    planes = (NV, LONG, SUB, CZ)
    near_state, own, ends, top, flag = pl.pallas_call(
        open_kernel,
        in_specs=[far] * 3,
        out_shape=(
            near(NV, ROWS, CZ), near(halves * n_z, NV * HALO + 1, CZ), near(NV, HALO, CY, CZ),
            near(NV, HALO, CX, CZ), pltpu.VMEM((CX, 1, CY), jnp.int32),
        ),
        scratch_shapes=[pltpu.SemaphoreType.DMA((NV + 2,))],
        compiler_params=ROOM, name="open",
    )(afar(flat), afar(top_ghost.transpose(0, 2, 1, 3)), afar(flags.transpose(0, 2, 1)))
    by_line = lax.all_to_all(held(own), ZLINE, 0, 0, tiled=True)
    relayed = pl.pallas_call(relay_kernel, out_shape=near(n_plane, 1, CZ), compiler_params=ROOM, name="relay")(held(by_line))
    speeds = lax.all_to_all(held(relayed), PLANE, 0, 0, tiled=True)
    ahead = [(i, i + 1) for i in range(n_plane - 1)]
    last = n_plane - 1

    def at(half, place, z):
        return (half * n_plane + place) * n_z + z

    soon = 3 if n_plane > 8 and n_z > 4 else 0
    seams, handed, passed = [], [], []
    for z in range(n_z):
        seams += [(at(1, 0, z), at(0, last, z)), (at(1, last, z), at(0, 0, z))]
        ends_of = ((0, last, 1 + z), (last, 0, last - 1 - z))
        for own_end, far_end, helper in ends_of:
            if z < soon:
                handed.append((at(0, own_end, z), at(0, helper, n_z - 1)))
                passed.append((at(0, helper, n_z - 1), at(1, far_end, z)))
            else:
                seams.append((at(0, own_end, z), at(1, far_end, z)))

    blocks = near_state.reshape(state.shape)
    upper, lower = blocks[:, CX - HALO :], blocks[:, :HALO]
    seam = lax.ppermute(ends, GX + ("gz",), seams)
    helped = lax.ppermute(ends, GX + ("gz",), handed)
    helped = lax.ppermute(helped, GX + ("gz",), passed)
    xhi = lax.ppermute(lower, PLANE, [(b, a) for a, b in ahead])
    xlo = lax.ppermute(upper, PLANE, ahead)

    peaks = pl.pallas_call(peak_kernel, out_shape=near(3, SUB, CZ), compiler_params=ROOM, name="peak")(held(speeds))

    new_state, new_register = pl.pallas_call(
        step_kernel,
        out_shape=(f32(NV, ROWS, CZ), f32(NV, ROWS, CZ)),
        in_specs=[close] * 9 + [far],
        out_specs=(far, far),
        scratch_shapes=[
            pltpu.VMEM(shape, jnp.float32)
            for shape in (
                (ROWS, CZ), (CY, CX, CZ), (NV, ROWS, CZ), planes, planes, planes, planes, (NV, CZ + 8, ROWS),
                (NV, 2 * HALO, CY, CZ), (NV, 2 * HALO, CY, CZ), (ROWS, CZ), (CZ, ROWS),
                (NV, ROWS, CZ), (NV, ROWS, CZ), (NV, ROWS, CZ),
            )
        ]
        + [
            pltpu.SemaphoreType.DMA((3, NV)),
        ],
        compiler_params=ROOM, name="step",
    )(
        *map(held, (peaks, near_state, xlo, xhi, seam, helped, by_line, top, flag)),
        afar(register.reshape(NV, ROWS, CZ)),
    )
    return (new_state.reshape(state.shape), new_register.reshape(state.shape))


def solution(mesh):
    finer = Mesh(
        mesh.devices.reshape(2, 8, 4, 2, mesh.shape["gz"]), ("gx_0", "gx_1", "gx_2", "gx_3", "gz")
    )
    placed = P(None, GX, None, "gz")
    return jax.shard_map(
        advance,
        mesh=finer,
        in_specs=(placed, placed, placed, P(GX, None, "gz")),
        out_specs=(placed, placed),
        check_vma=False,
    )
```

```python
import jax
import jax.numpy as jnp
from jax import lax
from jax.experimental import pallas as pl
from jax.experimental.pallas import tpu as pltpu
from jax.sharding import Mesh
from jax.sharding import PartitionSpec as P

GX = ("gx_0", "gx_1", "gx_2", "gx_3")
PLANE = ("gx_1", "gx_2", "gx_3")
ZLINE = ("gx_0", "gz")

GAMMA = 1.4
EPS_WENO = 1e-06
LAMBDA = (0.1, 0.15, 0.1)
REGISTER_DECAY = -5.0 / 9.0
UPDATE_WEIGHT = 15.0 / 16.0

NV = 5
CX = 8
CY = 16
CZ = 128
ROWS = CX * CY
HALO = 3
SUB = 8
LONG = 16 + 2 * HALO


def primitives(cons):
    inverse = 1.0 / cons[0]
    vels = [cons[k] * inverse for k in (1, 2, 3)]
    kinetic = cons[1] * vels[0] + cons[2] * vels[1] + cons[3] * vels[2]
    pressure = (GAMMA - 1.0) * (cons[4] - 0.5 * kinetic)
    return inverse, vels, pressure


def fetch(pairs, sems):
    copies = [pltpu.make_async_copy(src, dst, sems.at[i]) for i, (src, dst) in enumerate(pairs)]
    for copy in copies:
        copy.start()
    for copy in copies:
        copy.wait()


def line_neighbours():
    n_z, here = lax.axis_size("gz"), lax.axis_index("gz")
    first = lax.axis_index("gx_0") * n_z
    return first + lax.rem(here + n_z - 1, n_z), first + lax.rem(here + 1, n_z)


def open_kernel(
    far_ref, far_top_ref, far_flag_ref, state_ref, out_ref, ends_ref, top_ref, flag_ref, sems
):
    pairs = [(far_ref.at[v], state_ref.at[v]) for v in range(NV)]
    fetch(pairs + [(far_top_ref, top_ref), (far_flag_ref, flag_ref)], sems)
    best = [None] * 3
    for block in range(ROWS // SUB):
        rows = slice(block * SUB, block * SUB + SUB)
        inverse, vels, pressure = primitives([state_ref[v, rows, :] for v in range(NV)])
        sound = jnp.sqrt(GAMMA * pressure * inverse)
        for k in range(3):
            speed = jnp.abs(vels[k]) + sound
            best[k] = speed if block == 0 else jnp.maximum(best[k], speed)
    lane = lax.broadcasted_iota(jnp.int32, (1, CZ), 1)
    packed = jnp.zeros((1, CZ), jnp.float32)
    for k in range(3):
        top = jnp.max(jnp.max(best[k], axis=0, keepdims=True), axis=1, keepdims=True)
        packed = jnp.where(lane == k, top, packed)
    firsts, lasts = [], []
    for v in range(NV):
        turned = state_ref[v].T
        firsts.append(turned[:HALO])
        lasts.append(turned[CZ - HALO :])
    _, after = line_neighbours()
    for to in range(out_ref.shape[0]):
        forward = after == to
        for v in range(NV):
            out_ref[to, v * HALO : v * HALO + HALO, :] = jnp.where(forward, lasts[v], firsts[v])
        out_ref[to, NV * HALO : NV * HALO + 1, :] = packed
    first = plane_place()[0] == 0
    for v in range(NV):
        for i in range(HALO):
            for h in range(CY // SUB):
                low, high = i * CY + h * SUB, (CX - HALO + i) * CY + h * SUB
                ends_ref[v, i, h * SUB : h * SUB + SUB, :] = jnp.where(
                    first, state_ref[v, low : low + SUB, :], state_ref[v, high : high + SUB, :]
                )


def plane_place():
    place, last = 0, 1
    for axis in PLANE:
        place = place * lax.axis_size(axis) + lax.axis_index(axis)
        last = last * lax.axis_size(axis)
    return place, last - 1


def relay_kernel(got_ref, out_ref):
    row = slice(NV * HALO, NV * HALO + 1)
    best = got_ref[0, row, :]
    for i in range(1, got_ref.shape[0]):
        best = jnp.maximum(best, got_ref[i, row, :])
    for to in range(out_ref.shape[0]):
        out_ref[to] = best


def peak_kernel(speed_ref, out_ref):
    best = speed_ref[0]
    for i in range(1, speed_ref.shape[0]):
        best = jnp.maximum(best, speed_ref[i])
    lane = lax.broadcasted_iota(jnp.int32, (1, CZ), 1)
    for k in range(3):
        top = jnp.max(jnp.where(lane == k, best, 0.0), axis=1, keepdims=True)
        out_ref[k] = jnp.broadcast_to(top, (SUB, CZ))


def flux_of(cons, var):
    _, vels, pressure = primitives(cons)
    velocity = vels[var - 1]
    flux = [(cons[v] + pressure if v == 4 else cons[v]) * velocity for v in range(NV)]
    flux[var] = flux[var] + pressure
    return flux


def linear_parts(flux, cons, masks, scale):
    count = len(flux) - 2 * HALO

    def face(j):
        inner, outer = flux[j + 2] + flux[j + 3], flux[j + 1] + flux[j + 4]
        central = 37.0 * inner - 8.0 * outer + (flux[j] + flux[j + 5])
        return central, 7.0 * inner - outer, (cons[j + 4] - cons[j + 1]) - 3.0 * (cons[j + 3] - cons[j + 2])

    faces = [face(j) for j in range(count + 1)]
    base, tilt = [], []
    for low, high, mask in zip(faces, faces[1:], masks):
        base.append(jnp.where(mask, (scale / 12.0) * (high[1] - low[1]), (scale / 60.0) * (high[0] - low[0])))
        tilt.append(jnp.where(mask, (scale / 12.0) * (high[2] - low[2]), 0.0))
    return base, tilt


EPS_SCALED = 4.0 * EPS_WENO
CURVE = 4.0 / 3.0


def bent_faces(flux, cons, alpha):
    count = len(flux) - 2 * HALO + 1
    moved = [alpha * u for u in cons]

    def slopes(vals):
        step = [b - a for a, b in zip(vals, vals[1:])]
        bend = [None] + [b - a for a, b in zip(step, step[1:])]
        turn = [None] + [b - a for a, b in zip(bend[1:], bend[2:])]
        base = [None] + [CURVE * (d * d) + EPS_SCALED for d in bend[1:]]
        return step, bend, turn, base

    def pull(beta_a, beta_b, beta_c, near_turn, far_turn):
        u, w = beta_b / beta_a, beta_b / beta_c
        u, w = u * u, w * w
        w = 3.0 * w
        return ((u + u) * near_turn + w * far_turn) / (6.0 + u + w)

    pe, pd, pt, pk = slopes([f + m for f, m in zip(flux, moved)])
    me, md, mt, mk = slopes([f - m for f, m in zip(flux, moved)])
    out = []
    for j in range(count):
        bc, cd = pe[j + 1], pe[j + 2]
        plus = pull(
            pk[j + 1] + bc * (bc + pd[j + 1]), pk[j + 2] + bc * cd, pk[j + 3] + cd * (cd - pd[j + 3]), pt[j + 1], pt[j + 2]
        )
        bc, cd = me[j + 3], me[j + 2]
        minus = pull(
            mk[j + 4] + bc * (bc - md[j + 4]), mk[j + 3] + bc * cd, mk[j + 2] + cd * (cd + md[j + 2]), mt[j + 3], mt[j + 2]
        )
        out.append(minus - plus)
    return out


def prepare_kernel(state_ref, top_ref, flag_ref, xmask_ref, yf_ref, yu_ref, ybase_ref, ytilt_ref):
    square = (CY, CY)
    diagonal = lax.broadcasted_iota(jnp.int32, square, 0) == lax.broadcasted_iota(jnp.int32, square, 1)
    for x in range(CX):
        spread = jnp.broadcast_to(flag_ref[x].astype(jnp.float32), square)
        column = jnp.max(jnp.where(diagonal, spread, 0.0), axis=1, keepdims=True)
        xmask_ref[x * CY : x * CY + CY, :] = jnp.broadcast_to(column, (CY, CZ)) * (LAMBDA[0] / 12.0)

    def keep(to, cons, var, flux_ref, cons_ref):
        flux = flux_of(cons, var)
        for v in range(NV):
            flux_ref[v, to] = flux[v]
            cons_ref[v, to] = cons[v]

    for i in range(CY):
        cons = [state_ref[v, pl.ds(i, CX, stride=CY), :] for v in range(NV)]
        keep(i + HALO, cons, 2, yf_ref, yu_ref)
        if i < HALO:
            keep(HALO - 1 - i, [-c if v == 2 else c for v, c in enumerate(cons)], 2, yf_ref, yu_ref)
            keep(HALO + CY + i, [top_ref[v, i] for v in range(NV)], 2, yf_ref, yu_ref)
    masks = [xmask_ref[pl.ds(i, CX, stride=CY), :] > 0.0 for i in range(CY)]

    def per_var(v, carry):
        planes = range(LONG)
        base, tilt = linear_parts([yf_ref[v, i] for i in planes], [yu_ref[v, i] for i in planes], masks, LAMBDA[1])
        for i in range(CY):
            ybase_ref[v, i] = base[i]
            ytilt_ref[v, i] = tilt[i]
        return carry

    lax.fori_loop(0, NV, per_var, 0)


def step_kernel(
    speed_ref, state_ref, xlo_ref, xhi_ref, seam_ref, helped_ref, got_ref,
    xmask_ref, yf_ref, yu_ref, ybase_ref, ytilt_ref, old_reg_ref,
    far_state_ref, far_reg_ref,
    ymask_ref, xf_ref, zf_ref, zu_ref, line, side_f, side_u, acc_y, acc_z,
    reg_ref, state_out, reg_out, sems,
):
    def load(v):
        return pltpu.make_async_copy(old_reg_ref.at[v], reg_ref.at[v], sems.at[2, v])

    for v in range(NV):
        load(v).start()

    for y in range(CY):
        ymask_ref[y] = xmask_ref[pl.ds(y, CX, stride=CY), :] * (LAMBDA[1] / LAMBDA[0])
    zmask = xmask_ref[...].T[:SUB] * (LAMBDA[2] / LAMBDA[0])

    before, after = line_neighbours()
    for v in range(NV):
        rows = slice(v * HALO, v * HALO + HALO)
        line[v, :HALO, :] = got_ref[before, rows, :]
        line[v, HALO : HALO + CZ, :] = state_ref[v].T
        line[v, HALO + CZ : 2 * HALO + CZ, :] = got_ref[after, rows, :]

    def keep(to, cons, var, flux_ref, cons_ref):
        flux = flux_of(cons, var)
        for v in range(NV):
            flux_ref[v, to] = flux[v]
            cons_ref[v, to] = cons[v]

    for i in range(LONG):
        keep(i, [line[v, pl.ds(i, SUB, stride=CZ // SUB), :] for v in range(NV)], 3, zf_ref, zu_ref)


    alphas = [speed_ref[k] for k in range(3)]
    halves = [slice(h * SUB, h * SUB + SUB) for h in range(CY // SUB)]

    place, last = plane_place()
    for i in range(HALO):
        for rows in halves:
            for at, side_ref, end in ((i, xlo_ref, 0), (HALO + i, xhi_ref, last)):
                cons = [
                    jnp.where(
                        place == end, seam_ref[v, i, rows, :] + helped_ref[v, i, rows, :], side_ref[v, i, rows, :]
                    )
                    for v in range(NV)
                ]
                flux = flux_of(cons, 1)
                for v in range(NV):
                    side_f[v, at, rows, :] = flux[v]
                    side_u[v, at, rows, :] = cons[v]

    for block in range(ROWS // SUB):
        rows = slice(block * SUB, block * SUB + SUB)
        flux = flux_of([state_ref[v, rows, :] for v in range(NV)], 1)
        for v in range(NV):
            xf_ref[v, rows, :] = flux[v]

    def copies(v):
        return [
            pltpu.make_async_copy(state_out.at[v], far_state_ref.at[v], sems.at[0, v]),
            pltpu.make_async_copy(reg_out.at[v], far_reg_ref.at[v], sems.at[1, v]),
        ]

    def per_var(v, carry):
        flux, cons = [zf_ref[v, i] for i in range(LONG)], [zu_ref[v, i] for i in range(LONG)]
        bent = bent_faces(flux, cons, alphas[2])
        base, tilt = linear_parts(flux, cons, [zmask > 0.0] * CY, LAMBDA[2])
        for i in range(CY):
            acc_z[pl.ds(i, SUB, stride=CZ // SUB), :] = (
                base[i] + alphas[2] * tilt[i] + zmask * (bent[i + 1] - bent[i])
            )
        flux, cons = [yf_ref[v, i] for i in range(LONG)], [yu_ref[v, i] for i in range(LONG)]
        bent = bent_faces(flux, cons, alphas[1])
        for i in range(CY):
            acc_y[pl.ds(i, CX, stride=CY), :] = (
                ybase_ref[v, i] + alphas[1] * ytilt_ref[v, i] + ymask_ref[i] * (bent[i + 1] - bent[i])
            )
        spread = acc_z[...].T
        load(v).wait()
        for rows in halves:
            at = [slice(i * CY + rows.start, i * CY + rows.stop) for i in range(CX)]
            flux = (
                [side_f[v, i, rows, :] for i in range(HALO)]
                + [xf_ref[v, here, :] for here in at]
                + [side_f[v, HALO + i, rows, :] for i in range(HALO)]
            )
            cons = (
                [side_u[v, i, rows, :] for i in range(HALO)]
                + [state_ref[v, here, :] for here in at]
                + [side_u[v, HALO + i, rows, :] for i in range(HALO)]
            )
            bent = bent_faces(flux, cons, alphas[0])
            base, tilt = linear_parts(flux, cons, [xmask_ref[here, :] > 0.0 for here in at], LAMBDA[0])
            for i, here in enumerate(at):
                x_part = base[i] + alphas[0] * tilt[i] + xmask_ref[here, :] * (bent[i + 1] - bent[i])
                change = x_part + acc_y[here, :] + spread[here]
                register = REGISTER_DECAY * reg_ref[v, here, :] - change
                reg_out[v, here, :] = register
                state_out[v, here, :] = state_ref[v, here, :] + UPDATE_WEIGHT * register
        for copy in copies(v):
            copy.start()
        return carry

    lax.fori_loop(0, NV, per_var, 0)
    for v in range(NV):
        for copy in copies(v):
            copy.wait()


def f32(*shape):
    return jax.ShapeDtypeStruct(shape, jnp.float32)


def near(*shape):
    return pltpu.VMEM(shape, jnp.float32)


ROOM = pltpu.CompilerParams(vmem_limit_bytes=16 * 1024 * 1024)


def held(value):
    return pltpu.with_memory_space_constraint(value, pltpu.VMEM)


def afar(value):
    return pltpu.with_memory_space_constraint(value, pltpu.HBM)


def advance(state, register, top_ghost, flags):
    flat = state.reshape(NV, ROWS, CZ)
    halves, n_z = lax.axis_size("gx_0"), lax.axis_size("gz")
    n_plane = lax.axis_size("gx_1") * lax.axis_size("gx_2") * lax.axis_size("gx_3")

    far = pl.BlockSpec(memory_space=pltpu.HBM)
    close = pl.BlockSpec(memory_space=pltpu.VMEM)
    planes = (NV, LONG, SUB, CZ)
    near_state, own, ends, top, flag = pl.pallas_call(
        open_kernel,
        in_specs=[far] * 3,
        out_shape=(
            near(NV, ROWS, CZ), near(halves * n_z, NV * HALO + 1, CZ), near(NV, HALO, CY, CZ),
            near(NV, HALO, CX, CZ), pltpu.VMEM((CX, 1, CY), jnp.int32),
        ),
        scratch_shapes=[pltpu.SemaphoreType.DMA((NV + 2,))],
        compiler_params=ROOM, name="open",
    )(afar(flat), afar(top_ghost.transpose(0, 2, 1, 3)), afar(flags.transpose(0, 2, 1)))
    by_line = lax.all_to_all(held(own), ZLINE, 0, 0, tiled=True)
    strips = (NV, CY, SUB, CZ)
    xmask, yf, yu, ybase, ytilt = pl.pallas_call(
        prepare_kernel,
        out_shape=(near(ROWS, CZ), near(*planes), near(*planes), near(*strips), near(*strips)),
        compiler_params=ROOM, name="prepare",
    )(held(near_state), held(top), held(flag))
    relayed = pl.pallas_call(relay_kernel, out_shape=near(n_plane, 1, CZ), compiler_params=ROOM, name="relay")(held(by_line))
    speeds = lax.all_to_all(held(relayed), PLANE, 0, 0, tiled=True)
    ahead = [(i, i + 1) for i in range(n_plane - 1)]
    last = n_plane - 1

    def at(half, place, z):
        return (half * n_plane + place) * n_z + z

    soon = 3 if n_plane > 8 and n_z > 4 else 0
    seams, handed, passed = [], [], []
    for z in range(n_z):
        seams += [(at(1, 0, z), at(0, last, z)), (at(1, last, z), at(0, 0, z))]
        ends_of = ((0, last, 1 + z), (last, 0, last - 1 - z))
        for own_end, far_end, helper in ends_of:
            if z < soon:
                handed.append((at(0, own_end, z), at(0, helper, n_z - 1)))
                passed.append((at(0, helper, n_z - 1), at(1, far_end, z)))
            else:
                seams.append((at(0, own_end, z), at(1, far_end, z)))

    blocks = near_state.reshape(state.shape)
    upper, lower = blocks[:, CX - HALO :], blocks[:, :HALO]
    seam = lax.ppermute(ends, GX + ("gz",), seams)
    helped = lax.ppermute(ends, GX + ("gz",), handed)
    helped = lax.ppermute(helped, GX + ("gz",), passed)
    xhi = lax.ppermute(lower, PLANE, [(b, a) for a, b in ahead])
    xlo = lax.ppermute(upper, PLANE, ahead)

    peaks = pl.pallas_call(peak_kernel, out_shape=near(3, SUB, CZ), compiler_params=ROOM, name="peak")(held(speeds))

    new_state, new_register = pl.pallas_call(
        step_kernel,
        out_shape=(f32(NV, ROWS, CZ), f32(NV, ROWS, CZ)),
        in_specs=[close] * 12 + [far],
        out_specs=(far, far),
        scratch_shapes=[
            pltpu.VMEM(shape, jnp.float32)
            for shape in (
                (CY, CX, CZ), (NV, ROWS, CZ), planes, planes, (NV, CZ + 8, ROWS),
                (NV, 2 * HALO, CY, CZ), (NV, 2 * HALO, CY, CZ), (ROWS, CZ), (CZ, ROWS),
                (NV, ROWS, CZ), (NV, ROWS, CZ), (NV, ROWS, CZ),
            )
        ]
        + [
            pltpu.SemaphoreType.DMA((3, NV)),
        ],
        compiler_params=ROOM, name="step",
    )(
        *map(held, (peaks, near_state, xlo, xhi, seam, helped, by_line, xmask, yf, yu, ybase, ytilt)),
        afar(register.reshape(NV, ROWS, CZ)),
    )
    return (new_state.reshape(state.shape), new_register.reshape(state.shape))


def solution(mesh):
    finer = Mesh(
        mesh.devices.reshape(2, 8, 4, 2, mesh.shape["gz"]), ("gx_0", "gx_1", "gx_2", "gx_3", "gz")
    )
    placed = P(None, GX, None, "gz")
    return jax.shard_map(
        advance,
        mesh=finer,
        in_specs=(placed, placed, placed, P(GX, None, "gz")),
        out_specs=(placed, placed),
        check_vma=False,
    )
```
